32 devices in a mesh: pool: 32 (over z, y, x, core).
Axes of the slice: x: 2, y: 2, z: 4, core: 2. Of those that a mesh axis runs over, the one named last changes fastest.
Arguments:
- queries: bfloat16 [256, 32, 32, 128], P('pool')
- k_new: bfloat16 [256, 32, 8, 128], P('pool')
- v_new: bfloat16 [256, 32, 8, 128], P('pool')
- k_pool: bfloat16 [8192, 16, 8, 128], P('pool')
- v_pool: bfloat16 [8192, 16, 8, 128], P('pool')
- block_table: int32 [256, 64], replicated
- write_ids: int32 [256, 2], P('pool')
Outputs:
- output 1: bfloat16 [256, 32, 32, 128], P('pool')
- output 2: bfloat16 [8192, 16, 8, 128], P('pool')
- output 3: bfloat16 [8192, 16, 8, 128], P('pool')
All inputs are finite; a program needn't handle non-finite values.
Results may differ from the reference program's by a relative error of at most 0.0108546.
Values are sent between devices in bfloat16 or wider.
A program may use at most 1 GiB of HBM per device.

```python
import jax
import jax.numpy as jnp
from jax import lax

NUM_DEVICES = 32
REQ_PER_DEV = 8
CHUNK_LEN = 32
PREFIX_BLOCKS = 64
BLOCKS_PER_DEV = 256
BLOCK_LEN = 16
Q_HEADS = 32
KV_HEADS = 8
HEAD_DIM = 128


def draw_tables(rng_key):
    key_first, key_choice, key_start, key_base, key_write = jax.random.split(rng_key, 5)
    quarter = BLOCKS_PER_DEV // 4
    half_len = PREFIX_BLOCKS // 2
    per_owner = 2 * PREFIX_BLOCKS // NUM_DEVICES
    first_dev = jax.random.randint(key_first, (), 0, NUM_DEVICES)
    dev_choice = jax.random.randint(key_choice, (NUM_DEVICES,), 0, 2)
    win_start = first_dev + jax.random.randint(key_start, (NUM_DEVICES,), 0, NUM_DEVICES // 4)
    row_base = jax.random.randint(key_base, (NUM_DEVICES, REQ_PER_DEV), 0, quarter)
    slot_idx = jnp.arange(half_len)
    pop_owner = (first_dev + slot_idx // per_owner) % NUM_DEVICES
    pop_local = dev_choice[:, None] * per_owner + slot_idx[None, :] % per_owner
    pop_ids = pop_owner[None, :] * BLOCKS_PER_DEV + pop_local
    pop_rows = jnp.broadcast_to(pop_ids[:, None, :], (NUM_DEVICES, REQ_PER_DEV, half_len))
    win_owner = (win_start[:, None] + slot_idx[None, :]) % NUM_DEVICES
    win_local = quarter + (row_base[:, :, None] + slot_idx[None, None, :] // NUM_DEVICES) % quarter
    win_rows = win_owner[:, None, :] * BLOCKS_PER_DEV + win_local
    block_tab = jnp.concatenate([pop_rows, win_rows], axis=-1)
    block_tab = block_tab.reshape(NUM_DEVICES * REQ_PER_DEV, PREFIX_BLOCKS)
    new_blocks = REQ_PER_DEV * CHUNK_LEN // BLOCK_LEN
    write_keys = jax.random.split(key_write, NUM_DEVICES)
    shuffled = jax.vmap(lambda one_key: jax.random.permutation(one_key, BLOCKS_PER_DEV // 2))(write_keys)
    write_tab = shuffled[:, :new_blocks] + BLOCKS_PER_DEV // 2
    write_tab = write_tab.reshape(NUM_DEVICES * REQ_PER_DEV, CHUNK_LEN // BLOCK_LEN)
    return block_tab.astype(jnp.int32), write_tab.astype(jnp.int32)


def setup_inputs(seed: int = 0) -> dict:
    key_q, key_kn, key_vn, key_kp, key_vp, key_tab = jax.random.split(jax.random.key(seed), 6)
    n_rows = NUM_DEVICES * REQ_PER_DEV
    chunk_kv = (n_rows, CHUNK_LEN, KV_HEADS, HEAD_DIM)
    pool_shape = (NUM_DEVICES * BLOCKS_PER_DEV, BLOCK_LEN, KV_HEADS, HEAD_DIM)
    queries = jax.random.normal(key_q, (n_rows, CHUNK_LEN, Q_HEADS, HEAD_DIM), jnp.float32)
    k_new = jax.random.normal(key_kn, chunk_kv, jnp.float32)
    v_new = jax.random.normal(key_vn, chunk_kv, jnp.float32)
    k_pool = jax.random.normal(key_kp, pool_shape, jnp.float32)
    v_pool = jax.random.normal(key_vp, pool_shape, jnp.float32)
    block_table, write_ids = draw_tables(key_tab)
    return {'queries': queries.astype(jnp.bfloat16), 'k_new': k_new.astype(jnp.bfloat16), 'v_new': v_new.astype(jnp.bfloat16), 'k_pool': k_pool.astype(jnp.bfloat16), 'v_pool': v_pool.astype(jnp.bfloat16), 'block_table': block_table, 'write_ids': write_ids}


def attend_one(q_rows, k_all, v_all):
    groups = Q_HEADS // KV_HEADS
    prefix_len = PREFIX_BLOCKS * BLOCK_LEN
    q_grp = q_rows.astype(jnp.float32).reshape(CHUNK_LEN, KV_HEADS, groups, HEAD_DIM)
    scores = jnp.einsum('cgqd,tgd->cgqt', q_grp, k_all.astype(jnp.float32)) * HEAD_DIM ** -0.5
    visible = jnp.arange(prefix_len + CHUNK_LEN)[None, :] <= prefix_len + jnp.arange(CHUNK_LEN)[:, None]
    scores = jnp.where(visible[:, None, None, :], scores, -jnp.inf)
    prob_rows = jax.nn.softmax(scores, axis=-1).astype(jnp.bfloat16).astype(jnp.float32)
    attn_rows = jnp.einsum('cgqt,tgd->cgqd', prob_rows, v_all.astype(jnp.float32))
    return attn_rows.reshape(CHUNK_LEN, Q_HEADS, HEAD_DIM).astype(jnp.bfloat16)


def reference(queries, k_new, v_new, k_pool, v_pool, block_table, write_ids):
    prefix_len = PREFIX_BLOCKS * BLOCK_LEN
    n_rows = NUM_DEVICES * REQ_PER_DEV

    def one_request(row_item):
        q_rows, k_chunk, v_chunk, row_ids = row_item
        k_all = jnp.concatenate([k_pool[row_ids].reshape(prefix_len, KV_HEADS, HEAD_DIM), k_chunk], axis=0)
        v_all = jnp.concatenate([v_pool[row_ids].reshape(prefix_len, KV_HEADS, HEAD_DIM), v_chunk], axis=0)
        return attend_one(q_rows, k_all, v_all)

    attn_out = lax.map(one_request, (queries, k_new, v_new, block_table))
    targets = ((jnp.arange(n_rows) // REQ_PER_DEV)[:, None] * BLOCKS_PER_DEV + write_ids).reshape(-1)
    new_shape = (n_rows * CHUNK_LEN // BLOCK_LEN, BLOCK_LEN, KV_HEADS, HEAD_DIM)
    k_pool_out = k_pool.at[targets].set(k_new.reshape(new_shape))
    v_pool_out = v_pool.at[targets].set(v_new.reshape(new_shape))
    return attn_out, k_pool_out, v_pool_out
```

```python
import functools

import jax
import jax.numpy as jnp
from jax import lax
from jax.experimental import pallas as pl
from jax.experimental.pallas import tpu as pltpu
from jax.sharding import PartitionSpec as P

F32 = jnp.float32
BF16 = jnp.bfloat16
ROW_CAP = 5
POOL_CHUNK = 16
HOT_CAP = 64
MESH = pl.DeviceIdType.MESH


def any_spec():
    return pl.BlockSpec(memory_space=pl.ANY)


def smem_spec():
    return pl.BlockSpec(memory_space=pltpu.SMEM)


def vmem_spec():
    return pl.BlockSpec(memory_space=pltpu.VMEM)


def pack_pool_kernel(cfg, counts, near_ids, cross_ids, hot_ids, perm, k_pool, v_pool, x_near, x_cross, x_hot,
                     raw, head_major, zero, in_sem, out_sem, zero_sem):
    per_dev, n_half, pair_cap = cfg
    n_chunk = per_dev // POOL_CHUNK
    n_zero = HOT_CAP // POOL_CHUNK

    def chunk_copies(chunk, slot):
        rows = pl.ds(chunk * POOL_CHUNK, POOL_CHUNK)
        return (pltpu.make_async_copy(k_pool.at[rows], raw.at[slot, 0], in_sem.at[slot, 0]),
                pltpu.make_async_copy(v_pool.at[rows], raw.at[slot, 1], in_sem.at[slot, 1]))

    for copy in chunk_copies(0, 0):
        copy.start()
    zero[...] = jnp.zeros_like(zero)

    def turn_chunk(chunk, carry):
        slot = lax.rem(chunk, 2)

        @pl.when(chunk + 1 < n_chunk)
        def _():
            for copy in chunk_copies(chunk + 1, 1 - slot):
                copy.start()

        for copy in chunk_copies(chunk, slot):
            copy.wait()
        for j in range(POOL_CHUNK):
            both = jnp.concatenate([raw[slot, 0, j], raw[slot, 1, j]], axis=1)
            turned = jnp.dot(perm[...], both, preferred_element_type=F32).astype(BF16)
            head_major[chunk * POOL_CHUNK + j, 0:128, :] = turned[:, 0:128]
            head_major[chunk * POOL_CHUNK + j, 128:256, :] = turned[:, 128:256]

        @pl.when(chunk == 0)
        def _():
            for i in range(n_zero):
                pltpu.make_async_copy(zero, x_hot.at[pl.ds(i * POOL_CHUNK, POOL_CHUNK)], zero_sem.at[i]).start()
        return carry

    lax.fori_loop(0, n_chunk, turn_chunk, 0)

    def start_list(ids, row, count, dest, base):
        def body(k, carry):
            pltpu.make_async_copy(head_major.at[ids[row, k]], dest.at[base + k], out_sem).start()
            return carry
        lax.fori_loop(0, count, body, 0)

    start_list(cross_ids, 0, counts[n_half], x_cross, 0)
    total = counts[n_half] + counts[n_half + 1]
    for i in range(n_zero):
        pltpu.make_async_copy(zero, x_hot.at[pl.ds(i * POOL_CHUNK, POOL_CHUNK)], zero_sem.at[i]).wait()
    start_list(hot_ids, 0, counts[n_half + 1], x_hot, counts[n_half + 2])
    for q in range(n_half):
        start_list(near_ids, q, counts[q], x_near, q * pair_cap)
        total = total + counts[q]

    def drain(k, carry):
        pltpu.make_async_copy(head_major.at[0], x_near.at[0], out_sem).wait()
        return carry
    lax.fori_loop(0, total, drain, 0)


def pack_relay_kernel(cfg, counts, ids, arrived, x_out, stage, in_sem, out_sem):
    n_half, pair_cap, n_cross = cfg

    whole = pltpu.make_async_copy(arrived.at[pl.ds(0, n_cross)], stage, in_sem)
    whole.start()
    whole.wait()
    total = 0
    for q in range(n_half):
        def store(k, carry, q=q):
            pltpu.make_async_copy(stage.at[ids[q, k]], x_out.at[q * pair_cap + k], out_sem).start()
            return carry
        lax.fori_loop(0, counts[q], store, 0)
        total = total + counts[q]

    def drain(k, carry):
        pltpu.make_async_copy(stage.at[0], x_out.at[0], out_sem).wait()
        return carry
    lax.fori_loop(0, total, drain, 0)


def xor_bits(index, bits):
    out = index
    bit = 1
    while bit <= bits:
        if bits & bit:
            out = out + bit - 2 * bit * lax.rem(index // bit, 2)
        bit *= 2
    return out


def exchange_kernel(cfg, *refs):
    n_half, pair_cap, pair_send, n_cross, base = cfg
    if n_cross:
        x_near, x_cross, recv, arrived, own, send_sem, recv_sem, own_sem = refs
    else:
        x_near, _, recv, own, send_sem, recv_sem, own_sem = refs
    me = lax.axis_index('pool')
    in_half = lax.rem(me, n_half)
    half = me // n_half
    barrier = pltpu.get_barrier_semaphore()
    peers = [(j, half * n_half + xor_bits(in_half, j)) for j in range(1, n_half)]
    if n_cross:
        peers.append((n_half, (1 - half) * n_half + in_half))
    for _, peer in peers:
        pl.semaphore_signal(barrier, inc=1, device_id=(peer,), device_id_type=MESH)
    own_in = pltpu.make_async_copy(x_near.at[pl.ds(in_half * pair_cap, pair_send)], own, own_sem.at[0])
    own_in.start()
    pl.semaphore_wait(barrier, len(peers))
    copies = []
    for j, peer in reversed(peers):
        if j == n_half:
            src, dst = x_cross.at[pl.ds(0, n_cross)], arrived.at[pl.ds(0, n_cross)]
        else:
            src = x_near.at[pl.ds(xor_bits(in_half, j) * pair_cap, pair_send)]
            dst = recv.at[pl.ds((base + in_half) * pair_cap, pair_send)]
        copy = pltpu.make_async_remote_copy(
            src_ref=src, dst_ref=dst, send_sem=send_sem.at[j], recv_sem=recv_sem.at[j],
            device_id=(peer,), device_id_type=MESH)
        copy.start()
        copies.append(copy)
    own_in.wait()
    own_out = pltpu.make_async_copy(own, recv.at[pl.ds((base + in_half) * pair_cap, pair_send)], own_sem.at[1])
    own_out.start()
    own_out.wait()
    for copy in copies:
        copy.wait()


def attend_kernel(cfg, pos, q_ref, kn_ref, vn_ref, perm, recv, hot, out_ref, kv, heads_out, sem):
    n_pref, block_len, kv_heads, groups, chunk_len, head_dim, n_req, hot_base = cfg
    req = pl.program_id(0)
    slot = lax.rem(req, 2)
    exp_scale = float(head_dim ** -0.5 * 1.4426950408889634)

    def fetch(which, into):
        def body(k, carry):
            at = pos[which, k]

            @pl.when(at < hot_base)
            def _():
                pltpu.make_async_copy(recv.at[at], kv.at[into, k], sem.at[into]).start()

            @pl.when(at >= hot_base)
            def _():
                pltpu.make_async_copy(hot.at[at - hot_base], kv.at[into, k], sem.at[into]).start()
            return carry
        lax.fori_loop(0, n_pref, body, 0, unroll=8)

    @pl.when(req == 0)
    def _():
        fetch(0, 0)

    @pl.when(req + 1 < n_req)
    def _():
        fetch(req + 1, 1 - slot)

    pltpu.make_async_copy(recv.at[pl.ds(0, n_pref)], kv.at[slot], sem.at[slot]).wait()

    rows = chunk_len * groups
    token = lax.broadcasted_iota(jnp.int32, (rows, chunk_len), 0) // groups
    causal = lax.broadcasted_iota(jnp.int32, (rows, chunk_len), 1) <= token
    n_keys = n_pref * block_len
    nt = (((1,), (1,)), ((), ()))
    for h in range(kv_heads):
        q_h = q_ref[0, h]
        k_h = kv[slot, :, h * block_len:(h + 1) * block_len, :].reshape(n_keys, head_dim)
        v_at = (kv_heads + h) * block_len
        v_h = kv[slot, :, v_at:v_at + block_len, :].reshape(n_keys, head_dim)
        s_pref = lax.dot_general(q_h, k_h, nt, preferred_element_type=F32)
        s_self = lax.dot_general(q_h, kn_ref[0, h], nt, preferred_element_type=F32)
        s_self = jnp.where(causal, s_self, -jnp.inf)
        row_max = jnp.maximum(jnp.max(s_pref, axis=-1, keepdims=True), jnp.max(s_self, axis=-1, keepdims=True))
        e_pref = jnp.exp2((s_pref - row_max) * exp_scale)
        e_self = jnp.exp2((s_self - row_max) * exp_scale)
        total = jnp.sum(e_pref, axis=-1, keepdims=True) + jnp.sum(e_self, axis=-1, keepdims=True)
        inv = 1.0 / total
        p_pref = (e_pref * inv).astype(BF16)
        p_self = (e_self * inv).astype(BF16)
        acc = jnp.dot(p_pref, v_h, preferred_element_type=F32)
        acc = acc + jnp.dot(p_self, vn_ref[0, h], preferred_element_type=F32)
        heads_out[h] = acc.astype(BF16)
    span = 256 // kv_heads
    for g in range(rows // span):
        part = heads_out[:, g * span:(g + 1) * span, :].reshape(256, head_dim)
        out_ref[0, g * 256:(g + 1) * 256, :] = jnp.dot(perm[...], part, preferred_element_type=F32).astype(BF16)


def onehot(values, size):
    return (values[..., None] == jnp.arange(size, dtype=jnp.int32)).astype(BF16)


def ranks(ind):
    n = ind.shape[-1]
    strict = (jnp.arange(n)[:, None] < jnp.arange(n)[None, :]).astype(BF16)
    return jnp.einsum('...b,bk->...k', ind.astype(BF16), strict, preferred_element_type=F32).astype(jnp.int32)


def compact(ind, rank, value, size):
    hit = ind[..., :, None] & (rank[..., :, None] == jnp.arange(size))
    return jnp.sum(jnp.where(hit, value[..., :, None], 0), axis=-2)


def count(ind):
    return jnp.sum(ind.astype(jnp.int32), axis=-1)


def permutation(src_of_row):
    n = src_of_row.shape[0]
    return (src_of_row[:, None] == jnp.arange(n)[None, :]).astype(BF16)


def solution(mesh):
    n_dev = mesh.shape['pool']

    def local_step(queries, k_new, v_new, k_pool, v_pool, block_table, write_ids):
        req_count, chunk_len, q_heads, head_dim = queries.shape
        kv_heads = k_new.shape[2]
        groups = q_heads // kv_heads
        per_dev, block_len = k_pool.shape[0], k_pool.shape[1]
        n_pref = block_table.shape[1]
        block_rows = block_len * kv_heads
        pair_cap = req_count * ROW_CAP
        n_half = n_dev // 2
        hot_base = n_dev * pair_cap
        me = lax.axis_index('pool')
        half, partner = me // n_half, (me + n_half) % n_dev
        take = lambda x, at, axis: lax.dynamic_index_in_dim(x, at, axis, keepdims=False)

        table = block_table.reshape(n_dev, req_count * n_pref)
        want = jnp.einsum('deo,deb->dob', onehot(table // per_dev, n_dev), onehot(table % per_dev, per_dev),
                          preferred_element_type=F32) > 0
        popular = jnp.sum(want.astype(jnp.int32), axis=0)
        level_of = jnp.arange(2, n_dev + 2)
        at_least = jnp.sum((popular[None] >= level_of[:, None, None]).astype(jnp.int32), axis=(1, 2))
        threshold = 2 + jnp.sum((at_least > HOT_CAP).astype(jnp.int32))
        hot = popular >= threshold
        hot_count = count(hot)
        hot_start = jnp.cumsum(hot_count) - hot_count
        hot_rank = ranks(hot)
        rest = want & ~hot
        rank = ranks(rest)
        pair_count = count(rest)
        union = jnp.any(rest.reshape(2, n_half, n_dev, per_dev), axis=1)
        union_rank = ranks(union)
        union_count = count(union)
        other = (jnp.arange(2)[:, None] != jnp.arange(n_dev)[None, :] // n_half)
        pair_max = jnp.max(pair_count)
        union_max = jnp.max(jnp.where(other, union_count, 0))

        ids = jnp.arange(per_dev, dtype=jnp.int32)
        rest_half = lax.dynamic_slice_in_dim(rest, half * n_half, n_half, 0)
        rank_half = lax.dynamic_slice_in_dim(rank, half * n_half, n_half, 0)
        count_half = lax.dynamic_slice_in_dim(pair_count, half * n_half, n_half, 0)
        near_ids = compact(take(rest_half, me, 1), take(rank_half, me, 1), ids, pair_cap)
        relay_ids = compact(take(rest_half, partner, 1), take(rank_half, partner, 1),
                            take(take(union_rank, half, 0), partner, 0), pair_cap)
        cross_ids = compact(take(take(union, 1 - half, 0), me, 0), take(take(union_rank, 1 - half, 0), me, 0),
                            ids, per_dev)[None]
        hot_ids = compact(take(hot, me, 0), take(hot_rank, me, 0), ids, HOT_CAP)[None]
        counts = jnp.concatenate([take(count_half, me, 1), jnp.stack([
            union_count[1 - half, me], hot_count[me], hot_start[me]])])
        relay_counts = take(count_half, partner, 1)

        my_table = lax.dynamic_slice_in_dim(block_table, me * req_count, req_count, 0)
        owner = jnp.arange(n_dev)
        group = owner % n_half + jnp.where(owner // n_half == half, 0, n_half)
        place = jnp.where(hot, hot_base + hot_start[:, None] + hot_rank, group[:, None] * pair_cap + take(rank, me, 0))
        pos = place.reshape(-1)[my_table]

        block_shape = (2 * block_rows, head_dim)
        shaped = lambda n: jax.ShapeDtypeStruct((n,) + block_shape, BF16)
        row = jnp.arange(block_rows)
        turn = permutation((row % block_len) * kv_heads + row // block_len)
        x_near, x_cross, x_hot = pl.pallas_call(
            functools.partial(pack_pool_kernel, (per_dev, n_half, pair_cap)),
            out_shape=(shaped(n_half * pair_cap), shaped(per_dev), shaped(HOT_CAP)),
            in_specs=[smem_spec()] * 4 + [vmem_spec()] + [any_spec()] * 2,
            out_specs=(any_spec(),) * 3,
            scratch_shapes=[
                pltpu.VMEM((2, 2, POOL_CHUNK, block_rows, head_dim), BF16),
                pltpu.VMEM((per_dev,) + block_shape, BF16),
                pltpu.VMEM((POOL_CHUNK,) + block_shape, BF16),
                pltpu.SemaphoreType.DMA((2, 2)),
                pltpu.SemaphoreType.DMA,
                pltpu.SemaphoreType.DMA((HOT_CAP // POOL_CHUNK,)),
            ],
            compiler_params=pltpu.CompilerParams(vmem_limit_bytes=40 << 20),
            name='pack_pool',
        )(counts, near_ids, cross_ids, hot_ids, turn,
          k_pool.reshape(per_dev, block_rows, head_dim), v_pool.reshape(per_dev, block_rows, head_dim))

        rows = chunk_len * groups
        q_heads_major = queries.reshape(req_count, chunk_len, kv_heads, groups, head_dim)
        q_heads_major = q_heads_major.transpose(0, 2, 1, 3, 4).reshape(req_count, kv_heads, rows, head_dim)
        kn = k_new.transpose(0, 2, 1, 3)
        vn = v_new.transpose(0, 2, 1, 3)
        span_tok = 256 // q_heads
        out_row = jnp.arange(256)
        tok, head, grp = out_row // q_heads, (out_row % q_heads) // groups, out_row % groups
        back = permutation(head * (span_tok * groups) + tok * groups + grp)

        def exchange_and_attend(level, pair_send, n_cross, x_near, x_cross, x_hot, relay_counts, relay_ids, pos,
                                q_heads_major, kn, vn, back):
            hot_all = lax.psum(x_hot, 'pool')
            sems = [pltpu.VMEM((pair_send,) + block_shape, BF16), pltpu.SemaphoreType.DMA((n_half + 1,)),
                    pltpu.SemaphoreType.DMA((n_half + 1,)), pltpu.SemaphoreType.DMA((2,))]
            cost = lambda n: pl.CostEstimate(flops=n, bytes_accessed=1 << 20, transcendentals=0)
            recv, arrived = pl.pallas_call(
                functools.partial(exchange_kernel, (n_half, pair_cap, pair_send, n_cross, 0)),
                out_shape=(shaped(n_dev * pair_cap), shaped(n_cross)),
                in_specs=[any_spec()] * 2, out_specs=(any_spec(),) * 2, scratch_shapes=sems,
                compiler_params=pltpu.CompilerParams(collective_id=2 * level, has_side_effects=True,
                                                     vmem_limit_bytes=8 << 20),
                cost_estimate=cost(10 ** 10), name='exchange_near',
            )(x_near, x_cross)
            x_relay = pl.pallas_call(
                functools.partial(pack_relay_kernel, (n_half, pair_cap, n_cross)),
                out_shape=shaped(n_half * pair_cap),
                in_specs=[smem_spec()] * 2 + [any_spec()], out_specs=any_spec(),
                scratch_shapes=[pltpu.VMEM((n_cross,) + block_shape, BF16), pltpu.SemaphoreType.DMA,
                                pltpu.SemaphoreType.DMA],
                compiler_params=pltpu.CompilerParams(vmem_limit_bytes=24 << 20), name='pack_relay',
            )(relay_counts, relay_ids, arrived)
            recv = pl.pallas_call(
                functools.partial(exchange_kernel, (n_half, pair_cap, pair_send, 0, n_half)),
                out_shape=shaped(n_dev * pair_cap),
                in_specs=[any_spec()] * 2, out_specs=any_spec(), scratch_shapes=sems,
                input_output_aliases={1: 0},
                compiler_params=pltpu.CompilerParams(collective_id=2 * level + 1, has_side_effects=True,
                                                     vmem_limit_bytes=8 << 20),
                cost_estimate=cost(10 ** 10), name='exchange_far',
            )(x_relay, recv)
            cfg = (n_pref, block_len, kv_heads, groups, chunk_len, head_dim, req_count, hot_base)
            return pl.pallas_call(
                functools.partial(attend_kernel, cfg),
                out_shape=jax.ShapeDtypeStruct((req_count, chunk_len * q_heads, head_dim), BF16),
                grid=(req_count,),
                in_specs=[
                    smem_spec(),
                    pl.BlockSpec((1, kv_heads, rows, head_dim), lambda r: (r, 0, 0, 0)),
                    pl.BlockSpec((1, kv_heads, chunk_len, head_dim), lambda r: (r, 0, 0, 0)),
                    pl.BlockSpec((1, kv_heads, chunk_len, head_dim), lambda r: (r, 0, 0, 0)),
                    pl.BlockSpec((256, 256), lambda r: (0, 0)),
                    any_spec(), any_spec(),
                ],
                out_specs=pl.BlockSpec((1, chunk_len * q_heads, head_dim), lambda r: (r, 0, 0)),
                scratch_shapes=[
                    pltpu.VMEM((2, n_pref) + block_shape, BF16),
                    pltpu.VMEM((kv_heads, rows, head_dim), BF16),
                    pltpu.SemaphoreType.DMA((2,)),
                ],
                compiler_params=pltpu.CompilerParams(
                    vmem_limit_bytes=48 << 20, dimension_semantics=('arbitrary',)),
                name='attend',
            )(pos, q_heads_major, kn, vn, back, recv, hot_all)

        sizes = ((req_count, per_dev // 4), (req_count + req_count // 2, per_dev * 5 // 16), (pair_cap, per_dev))
        level = jnp.int32(0)
        for pair_send, n_cross in sizes[:-1]:
            level = level + ((pair_max > pair_send) | (union_max > n_cross)).astype(jnp.int32)
        attn = lax.switch(
            level, [functools.partial(exchange_and_attend, i, *s) for i, s in enumerate(sizes)],
            x_near, x_cross, x_hot, relay_counts, relay_ids, pos, q_heads_major, kn, vn, back)
        attn_out = attn.reshape(req_count, chunk_len, q_heads, head_dim)
        new_shape = (req_count * chunk_len // block_len, block_len, kv_heads, head_dim)
        targets = write_ids.reshape(-1)
        k_pool_out = k_pool.at[targets].set(k_new.reshape(new_shape))
        v_pool_out = v_pool.at[targets].set(v_new.reshape(new_shape))
        return attn_out, k_pool_out, v_pool_out

    row_spec = P('pool')
    return jax.shard_map(local_step, mesh=mesh, in_specs=(row_spec, row_spec, row_spec, row_spec, row_spec, P(), row_spec), out_specs=(row_spec, row_spec, row_spec), check_vma=False)
```

```python
import functools

import jax
import jax.numpy as jnp
from jax import lax
from jax.experimental import pallas as pl
from jax.experimental.pallas import tpu as pltpu
from jax.sharding import PartitionSpec as P

F32 = jnp.float32
BF16 = jnp.bfloat16
ROW_CAP = 5
POOL_CHUNK = 16
HOT_CAP = 64
PLANES = 4
HOT_PART = 4
HOT_IN = PLANES * HOT_PART
MESH = pl.DeviceIdType.MESH
LEVELS = ((8, 58, 10), (8, 64, 10), (12, 80, 16))


def any_spec():
    return pl.BlockSpec(memory_space=pl.ANY)


def smem_spec():
    return pl.BlockSpec(memory_space=pltpu.SMEM)


def vmem_spec():
    return pl.BlockSpec(memory_space=pltpu.VMEM)


def pack_pool_kernel(cfg, counts, near_ids, cross_ids, hot_ids, perm, k_pool, v_pool, x_near, x_cross, x_hot,
                     raw, head_major, in_sem, out_sem):
    per_dev, n_half, pair_cap = cfg
    n_chunk = per_dev // POOL_CHUNK

    def chunk_copies(chunk, slot):
        rows = pl.ds(chunk * POOL_CHUNK, POOL_CHUNK)
        return (pltpu.make_async_copy(k_pool.at[rows], raw.at[slot, 0], in_sem.at[slot, 0]),
                pltpu.make_async_copy(v_pool.at[rows], raw.at[slot, 1], in_sem.at[slot, 1]))

    for copy in chunk_copies(0, 0):
        copy.start()

    def turn_chunk(chunk, carry):
        slot = lax.rem(chunk, 2)

        @pl.when(chunk + 1 < n_chunk)
        def _():
            for copy in chunk_copies(chunk + 1, 1 - slot):
                copy.start()

        for copy in chunk_copies(chunk, slot):
            copy.wait()
        for j in range(POOL_CHUNK):
            both = jnp.concatenate([raw[slot, 0, j], raw[slot, 1, j]], axis=1)
            turned = jnp.dot(perm[...], both, preferred_element_type=F32).astype(BF16)
            head_major[chunk * POOL_CHUNK + j, 0:128, :] = turned[:, 0:128]
            head_major[chunk * POOL_CHUNK + j, 128:256, :] = turned[:, 128:256]
        return carry

    lax.fori_loop(0, n_chunk, turn_chunk, 0)

    def start_list(ids, row, count, dest, base):
        def body(k, carry):
            pltpu.make_async_copy(head_major.at[ids[row, k]], dest.at[base + k], out_sem).start()
            return carry
        lax.fori_loop(0, count, body, 0)

    start_list(cross_ids, 0, counts[n_half], x_cross, 0)
    total = counts[n_half]
    for q in range(2):
        start_list(hot_ids, q, counts[n_half + 1 + q], x_hot, q * HOT_PART)
        total = total + counts[n_half + 1 + q]
    for q in range(n_half):
        start_list(near_ids, q, counts[q], x_near, q * pair_cap)
        total = total + counts[q]

    def drain(k, carry):
        pltpu.make_async_copy(head_major.at[0], x_near.at[0], out_sem).wait()
        return carry
    lax.fori_loop(0, total, drain, 0)


def pack_relay_kernel(cfg, counts, ids, arrived, x_out, stage, in_sem, out_sem):
    n_half, far_cap, n_arrived = cfg

    whole = pltpu.make_async_copy(arrived, stage, in_sem)
    whole.start()
    whole.wait()
    total = 0
    for q in range(n_half):
        def store(k, carry, q=q):
            pltpu.make_async_copy(stage.at[ids[q, k]], x_out.at[q * far_cap + k], out_sem).start()
            return carry
        lax.fori_loop(0, counts[q], store, 0)
        total = total + counts[q]

    def drain(k, carry):
        pltpu.make_async_copy(stage.at[0], x_out.at[0], out_sem).wait()
        return carry
    lax.fori_loop(0, total, drain, 0)


def xor_bits(index, bits):
    out = index
    bit = 1
    while bit <= bits:
        if bits & bit:
            out = out + bit - 2 * bit * lax.rem(index // bit, 2)
        bit *= 2
    return out


def exchange_kernel(cfg, *refs):
    n_half, slot_cap, pair_send, n_cross, base = cfg
    first = n_cross > 0
    if first:
        x_pair, x_cross, x_hot, recv, arrived, own, send_sem, recv_sem, own_sem = refs
    else:
        x_pair, _, recv, own, send_sem, recv_sem, own_sem = refs
    me = lax.axis_index('pool')
    in_half = lax.rem(me, n_half)
    half = me // n_half
    n_cols = 2 * n_half // PLANES
    plane, col = me // n_cols, lax.rem(me, n_cols)
    own_group = recv.at[pl.ds(base + in_half * slot_cap, pair_send)]
    sends = []
    for j in range(1, n_half):
        sends.append((half * n_half + xor_bits(in_half, j),
                      x_pair.at[pl.ds(xor_bits(in_half, j) * slot_cap, pair_send)], own_group))
    own_copies = [(x_pair.at[pl.ds(in_half * slot_cap, pair_send)], own.at[pl.ds(0, pair_send)], own_group)]
    if first:
        hot_here = arrived.at[pl.ds(plane * HOT_PART, HOT_PART)]
        hot_for = lambda p: x_hot.at[pl.ds(lax.rem(p, 2) * HOT_PART, HOT_PART)]
        for j in range(1, PLANES):
            to = xor_bits(plane, j)
            sends.append((to * n_cols + col, hot_for(to), hot_here))
        sends.append(((1 - half) * n_half + in_half, x_cross.at[pl.ds(0, n_cross)],
                      arrived.at[pl.ds(HOT_IN, n_cross)]))
        own_copies.append((hot_for(plane), own.at[pl.ds(pair_send, HOT_PART)], hot_here))

    barrier = pltpu.get_barrier_semaphore()
    for peer, _, _ in sends:
        pl.semaphore_signal(barrier, inc=1, device_id=(peer,), device_id_type=MESH)
    own_in = [pltpu.make_async_copy(src, mid, own_sem.at[0, i]) for i, (src, mid, _) in enumerate(own_copies)]
    for copy in own_in:
        copy.start()
    pl.semaphore_wait(barrier, len(sends))
    copies = []
    for i, (peer, src, dst) in reversed(list(enumerate(sends))):
        copies.append(pltpu.make_async_remote_copy(
            src_ref=src, dst_ref=dst, send_sem=send_sem.at[i], recv_sem=recv_sem.at[i],
            device_id=(peer,), device_id_type=MESH))
        copies[-1].start()
    for copy in own_in:
        copy.wait()
    own_out = [pltpu.make_async_copy(mid, dst, own_sem.at[1, i]) for i, (_, mid, dst) in enumerate(own_copies)]
    for copy in own_out:
        copy.start()
    for copy in own_out + copies:
        copy.wait()


def attend_kernel(cfg, pos, targets, q_ref, kn_ref, vn_ref, perm, recv, k_pool, v_pool, k_new, v_new,
                  out_ref, k_out, v_out, kv, heads_out, sem, pool_buf, new_buf, pool_in, pool_done, new_sem):
    n_pref, block_len, kv_heads, groups, chunk_len, head_dim, n_req, per_dev, n_new = cfg
    req = pl.program_id(0)
    slot = lax.rem(req, 2)
    exp_scale = float(head_dim ** -0.5 * 1.4426950408889634)
    piece = 2 * per_dev // n_req

    def fetch(which, into):
        def body(k, carry):
            pltpu.make_async_copy(recv.at[pos[which, k]], kv.at[into, k], sem.at[into]).start()
            return carry
        lax.fori_loop(0, n_pref, body, 0, unroll=8)

    def pool_copies(step, at):
        rows = pl.ds(step * piece, piece)
        pairs = ((k_pool, k_out), (v_pool, v_out))
        return ([pltpu.make_async_copy(src.at[rows], pool_buf.at[at, i], pool_in.at[at, i])
                 for i, (src, _) in enumerate(pairs)],
                [pltpu.make_async_copy(pool_buf.at[at, i], dst.at[rows], pool_done.at[at, i])
                 for i, (_, dst) in enumerate(pairs)])

    new_in = [pltpu.make_async_copy(src, new_buf.at[i], new_sem.at[i]) for i, src in enumerate((k_new, v_new))]

    def new_out(i, which):
        dst = (k_out, v_out)[which]
        return pltpu.make_async_copy(new_buf.at[which, i], dst.at[targets[i]], new_sem.at[2])

    @pl.when(req == 0)
    def _():
        fetch(0, 0)
        for copy in pool_copies(0, 0)[0] + new_in:
            copy.start()

    @pl.when(req + 1 < n_req)
    def _():
        fetch(req + 1, 1 - slot)

    n_step = n_req // 2
    for step in range(n_step):
        @pl.when(req == step)
        def _(step=step):
            at = step % 2
            ins, outs = pool_copies(step, at)
            for copy in ins:
                copy.wait()
            for copy in outs:
                copy.start()
            if step + 1 < n_step:
                if step > 0:
                    for copy in pool_copies(step - 1, 1 - at)[1]:
                        copy.wait()
                for copy in pool_copies(step + 1, 1 - at)[0]:
                    copy.start()

    @pl.when(req == n_step)
    def _():
        for step in (n_step - 2, n_step - 1):
            for copy in pool_copies(step, step % 2)[1]:
                copy.wait()
        for copy in new_in:
            copy.wait()
        for i in range(n_new):
            new_out(i, 0).start()
            new_out(i, 1).start()

    @pl.when(req == n_req - 1)
    def _():
        for i in range(n_new):
            new_out(i, 0).wait()
            new_out(i, 1).wait()

    pltpu.make_async_copy(recv.at[pl.ds(0, n_pref)], kv.at[slot], sem.at[slot]).wait()

    rows = chunk_len * groups
    token = lax.broadcasted_iota(jnp.int32, (rows, chunk_len), 0) // groups
    causal = lax.broadcasted_iota(jnp.int32, (rows, chunk_len), 1) <= token
    n_keys = n_pref * block_len
    nt = (((1,), (1,)), ((), ()))
    for h in range(kv_heads):
        q_h = q_ref[0, h]
        k_h = kv[slot, :, h * block_len:(h + 1) * block_len, :].reshape(n_keys, head_dim)
        v_at = (kv_heads + h) * block_len
        v_h = kv[slot, :, v_at:v_at + block_len, :].reshape(n_keys, head_dim)
        s_pref = lax.dot_general(q_h, k_h, nt, preferred_element_type=F32)
        s_self = lax.dot_general(q_h, kn_ref[0, h], nt, preferred_element_type=F32)
        s_self = jnp.where(causal, s_self, -jnp.inf)
        row_max = jnp.maximum(jnp.max(s_pref, axis=-1, keepdims=True), jnp.max(s_self, axis=-1, keepdims=True))
        e_pref = jnp.exp2((s_pref - row_max) * exp_scale)
        e_self = jnp.exp2((s_self - row_max) * exp_scale)
        total = jnp.sum(e_pref, axis=-1, keepdims=True) + jnp.sum(e_self, axis=-1, keepdims=True)
        inv = 1.0 / total
        p_pref = (e_pref * inv).astype(BF16)
        p_self = (e_self * inv).astype(BF16)
        acc = jnp.dot(p_pref, v_h, preferred_element_type=F32)
        acc = acc + jnp.dot(p_self, vn_ref[0, h], preferred_element_type=F32)
        heads_out[h] = acc.astype(BF16)
    span = 256 // kv_heads
    for g in range(rows // span):
        part = heads_out[:, g * span:(g + 1) * span, :].reshape(256, head_dim)
        out_ref[0, g * 256:(g + 1) * 256, :] = jnp.dot(perm[...], part, preferred_element_type=F32).astype(BF16)


def onehot(values, size):
    return (values[..., None] == jnp.arange(size, dtype=jnp.int32)).astype(BF16)


def ranks(ind):
    n = ind.shape[-1]
    strict = (jnp.arange(n)[:, None] < jnp.arange(n)[None, :]).astype(BF16)
    return jnp.einsum('...b,bk->...k', ind.astype(BF16), strict, preferred_element_type=F32).astype(jnp.int32)


def compact(ind, rank, value, size):
    hit = ind[..., :, None] & (rank[..., :, None] == jnp.arange(size))
    return jnp.sum(jnp.where(hit, value[..., :, None], 0), axis=-2)


def count(ind):
    return jnp.sum(ind.astype(jnp.int32), axis=-1)


def flat_ranks(ind):
    per_row = count(ind)
    before = jnp.cumsum(per_row, axis=-1) - per_row
    return ranks(ind) + before[..., None], jnp.sum(per_row, axis=-1)


def permutation(src_of_row):
    n = src_of_row.shape[0]
    return (src_of_row[:, None] == jnp.arange(n)[None, :]).astype(BF16)


def solution(mesh):
    n_dev = mesh.shape['pool']

    def local_step(queries, k_new, v_new, k_pool, v_pool, block_table, write_ids):
        req_count, chunk_len, q_heads, head_dim = queries.shape
        kv_heads = k_new.shape[2]
        groups = q_heads // kv_heads
        per_dev, block_len = k_pool.shape[0], k_pool.shape[1]
        n_pref = block_table.shape[1]
        block_rows = block_len * kv_heads
        pair_cap = req_count * ROW_CAP
        n_half = n_dev // 2
        n_cols = n_dev // PLANES
        far_cap = pair_cap + HOT_IN
        far_base = n_half * pair_cap
        n_recv = far_base + n_half * far_cap
        me = lax.axis_index('pool')
        half, partner = me // n_half, (me + n_half) % n_dev
        take = lambda x, at, axis: lax.dynamic_index_in_dim(x, at, axis, keepdims=False)

        table = block_table.reshape(n_dev, req_count * n_pref)
        want = jnp.einsum('deo,deb->dob', onehot(table // per_dev, n_dev), onehot(table % per_dev, per_dev),
                          preferred_element_type=F32) > 0
        popular = jnp.sum(want.astype(jnp.int32), axis=0)
        level_of = jnp.arange(2, n_dev + 2)
        at_least = jnp.sum((popular[None] >= level_of[:, None, None]).astype(jnp.int32), axis=(1, 2))
        threshold = 2 + jnp.sum((at_least > HOT_CAP).astype(jnp.int32))
        hot = popular >= threshold
        hot_rank = ranks(hot)
        hot = hot & (hot_rank < 2 * HOT_PART)
        hot_part = jnp.where(hot, hot_rank % 2, 2)
        rest = want & ~hot
        rank = ranks(rest)
        pair_count = count(rest)
        union = jnp.any(rest.reshape(2, n_half, n_dev, per_dev), axis=1)
        union_rank = ranks(union)
        union_count = count(union)
        other = (jnp.arange(2)[:, None] != jnp.arange(n_dev)[None, :] // n_half)
        hot_want = want[:, None] & (hot_part == jnp.arange(2)[:, None, None])[None]
        hot_num = count(hot_want).reshape(n_dev, 2, PLANES, n_cols)
        far_hot = jnp.sum(hot_num, axis=2).reshape(n_dev, n_half)
        dest_half = jnp.arange(n_dev) // n_half
        far_rest = jnp.where(dest_half[:, None] == 0, pair_count[:, n_half:], pair_count[:, :n_half])
        pair_max = jnp.max(pair_count)
        far_max = jnp.max(far_rest + far_hot)
        union_max = jnp.max(jnp.where(other, union_count, 0))

        ids = jnp.arange(per_dev, dtype=jnp.int32)
        halved = lambda x: lax.dynamic_slice_in_dim(x, half * n_half, n_half, 0)
        rest_half, rank_half, count_half = halved(rest), halved(rank), halved(pair_count)
        near_ids = compact(take(rest_half, me, 1), take(rank_half, me, 1), ids, pair_cap)
        cross_ids = compact(take(take(union, 1 - half, 0), me, 0), take(take(union_rank, 1 - half, 0), me, 0),
                            ids, per_dev)[None]
        part_mine = take(hot_part, me, 0) == jnp.arange(2)[:, None]
        hot_ids = compact(part_mine, take(hot_rank, me, 0)[None] // 2, ids, HOT_PART)
        counts = jnp.concatenate([take(count_half, me, 1), union_count[1 - half, me][None], count(part_mine)])

        plane, col = me // n_cols, me % n_cols
        by_col = lambda x: x.reshape(x.shape[:-2] + (PLANES, n_cols, per_dev))
        hot_col = take(take(by_col(halved(hot_want)), plane % 2, 1), col, 2)
        hot_at = jnp.arange(PLANES)[:, None] * HOT_PART + take(by_col(hot_rank), col, 1) // 2
        relay_want = jnp.concatenate([take(rest_half, partner, 1)[:, None], hot_col], axis=1)
        relay_at = jnp.concatenate([HOT_IN + take(take(union_rank, half, 0), partner, 0)[None], hot_at], axis=0)
        relay_rank, relay_counts = flat_ranks(relay_want)
        n_flat = (PLANES + 1) * per_dev
        relay_ids = compact(relay_want.reshape(n_half, n_flat), relay_rank.reshape(n_half, n_flat),
                            relay_at.reshape(1, n_flat), far_cap)

        my_table = lax.dynamic_slice_in_dim(block_table, me * req_count, req_count, 0)
        owner = jnp.arange(n_dev)
        group = (owner % n_half)[:, None]
        my_rank = take(rank, me, 0)
        is_near = (owner // n_half == half)[:, None]
        place = jnp.where(is_near, group * pair_cap + my_rank, far_base + group * far_cap + my_rank)
        my_hot = by_col(take(hot_want, me, 0)).transpose(0, 2, 1, 3)
        my_hot_rank = flat_ranks(my_hot)[0].transpose(0, 2, 1, 3).reshape(2, n_dev, per_dev)
        my_hot_rank = jnp.where(hot_part == 0, my_hot_rank[0], my_hot_rank[1])
        holder = jnp.where(hot_part == 1, n_cols, 0) + (owner % n_cols)[:, None]
        my_far_rest = take(far_rest, me, 0).reshape(2, 1, n_cols)
        before = jnp.broadcast_to(my_far_rest, (2, PLANES, n_cols)).reshape(2, n_dev, 1)
        before = jnp.where(hot_part == 1, before[1], before[0])
        place = jnp.where(hot, far_base + holder * far_cap + before + my_hot_rank, place)
        pos = place.reshape(-1)[my_table]

        block_shape = (2 * block_rows, head_dim)
        shaped = lambda n: jax.ShapeDtypeStruct((n,) + block_shape, BF16)
        row = jnp.arange(block_rows)
        turn = permutation((row % block_len) * kv_heads + row // block_len)
        flat_pool = (per_dev, block_rows, head_dim)
        k_flat, v_flat = k_pool.reshape(flat_pool), v_pool.reshape(flat_pool)
        x_near, x_cross, x_hot = pl.pallas_call(
            functools.partial(pack_pool_kernel, (per_dev, n_half, pair_cap)),
            out_shape=(shaped(n_half * pair_cap), shaped(per_dev), shaped(2 * HOT_PART)),
            in_specs=[smem_spec()] * 4 + [vmem_spec()] + [any_spec()] * 2,
            out_specs=(any_spec(),) * 3,
            scratch_shapes=[
                pltpu.VMEM((2, 2, POOL_CHUNK, block_rows, head_dim), BF16),
                pltpu.VMEM((per_dev,) + block_shape, BF16),
                pltpu.SemaphoreType.DMA((2, 2)),
                pltpu.SemaphoreType.DMA,
            ],
            compiler_params=pltpu.CompilerParams(vmem_limit_bytes=40 << 20),
            name='pack_pool',
        )(counts, near_ids, cross_ids, hot_ids, turn, k_flat, v_flat)

        rows = chunk_len * groups
        q_heads_major = queries.reshape(req_count, chunk_len, kv_heads, groups, head_dim)
        q_heads_major = q_heads_major.transpose(0, 2, 1, 3, 4).reshape(req_count, kv_heads, rows, head_dim)
        kn = k_new.transpose(0, 2, 1, 3)
        vn = v_new.transpose(0, 2, 1, 3)
        span_tok = 256 // q_heads
        out_row = jnp.arange(256)
        tok, head, grp = out_row // q_heads, (out_row % q_heads) // groups, out_row % groups
        back = permutation(head * (span_tok * groups) + tok * groups + grp)

        def exchange(level, near_send, n_cross, far_send, x_near, x_cross, x_hot, relay_counts, relay_ids):
            n_arrived = HOT_IN + n_cross

            def exchange_call(first, send, out_shape, n_in, alias, name):
                n_copy = n_half + PLANES
                return pl.pallas_call(
                    functools.partial(exchange_kernel, (
                        n_half, pair_cap if first else far_cap, send, n_cross if first else 0,
                        0 if first else far_base)),
                    out_shape=out_shape, in_specs=[any_spec()] * n_in,
                    out_specs=(any_spec(),) * 2 if first else any_spec(),
                    scratch_shapes=[
                        pltpu.VMEM((send + HOT_PART,) + block_shape, BF16), pltpu.SemaphoreType.DMA((n_copy,)),
                        pltpu.SemaphoreType.DMA((n_copy,)), pltpu.SemaphoreType.DMA((2, 2))],
                    input_output_aliases=alias,
                    compiler_params=pltpu.CompilerParams(
                        collective_id=2 * level + (0 if first else 1), has_side_effects=True,
                        vmem_limit_bytes=8 << 20),
                    name=name)

            recv, arrived = exchange_call(True, near_send, (shaped(n_recv), shaped(n_arrived)), 3, {},
                                          'exchange_near')(x_near, x_cross, x_hot)
            x_relay = pl.pallas_call(
                functools.partial(pack_relay_kernel, (n_half, far_cap, n_arrived)),
                out_shape=shaped(n_half * far_cap),
                in_specs=[smem_spec()] * 2 + [any_spec()], out_specs=any_spec(),
                scratch_shapes=[pltpu.VMEM((n_arrived,) + block_shape, BF16), pltpu.SemaphoreType.DMA,
                                pltpu.SemaphoreType.DMA],
                compiler_params=pltpu.CompilerParams(vmem_limit_bytes=24 << 20), name='pack_relay',
            )(relay_counts, relay_ids, arrived)
            return exchange_call(False, far_send, shaped(n_recv), 2, {1: 0}, 'exchange_far')(x_relay, recv)

        sizes = tuple(LEVELS) + ((pair_cap, per_dev, far_cap),)
        level = jnp.int32(0)
        for near_send, n_cross, far_send in LEVELS:
            over = (pair_max > near_send) | (union_max > n_cross) | (far_max > far_send)
            level = level + over.astype(jnp.int32)
        recv = lax.switch(level, [functools.partial(exchange, i, *s) for i, s in enumerate(sizes)],
                          x_near, x_cross, x_hot, relay_counts, relay_ids)

        cfg = (n_pref, block_len, kv_heads, groups, chunk_len, head_dim, req_count, per_dev, write_ids.size)
        new_shape = (write_ids.size, block_rows, head_dim)
        row_block = lambda *dims: pl.BlockSpec((1,) + dims, lambda r: (r,) + (0,) * len(dims))
        attn, k_pool_out, v_pool_out = pl.pallas_call(
            functools.partial(attend_kernel, cfg),
            out_shape=(jax.ShapeDtypeStruct((req_count, chunk_len * q_heads, head_dim), BF16),
                       jax.ShapeDtypeStruct(flat_pool, BF16), jax.ShapeDtypeStruct(flat_pool, BF16)),
            grid=(req_count,),
            in_specs=[
                smem_spec(), smem_spec(), row_block(kv_heads, rows, head_dim), row_block(kv_heads, chunk_len, head_dim),
                row_block(kv_heads, chunk_len, head_dim), pl.BlockSpec((256, 256), lambda r: (0, 0)),
            ] + [any_spec()] * 5,
            out_specs=(row_block(chunk_len * q_heads, head_dim), any_spec(), any_spec()),
            scratch_shapes=[
                pltpu.VMEM((2, n_pref) + block_shape, BF16),
                pltpu.VMEM((kv_heads, rows, head_dim), BF16),
                pltpu.SemaphoreType.DMA((2,)),
                pltpu.VMEM((2, 2, 2 * per_dev // req_count, block_rows, head_dim), BF16),
                pltpu.VMEM((2,) + new_shape, BF16),
                pltpu.SemaphoreType.DMA((2, 2)),
                pltpu.SemaphoreType.DMA((2, 2)),
                pltpu.SemaphoreType.DMA((3,)),
            ],
            compiler_params=pltpu.CompilerParams(
                vmem_limit_bytes=56 << 20, dimension_semantics=('arbitrary',)),
            name='attend',
        )(pos, write_ids.reshape(-1), q_heads_major, kn, vn, back, recv, k_flat, v_flat,
          k_new.reshape(new_shape), v_new.reshape(new_shape))
        attn_out = attn.reshape(req_count, chunk_len, q_heads, head_dim)
        return attn_out, k_pool_out.reshape(k_pool.shape), v_pool_out.reshape(v_pool.shape)

    row_spec = P('pool')
    return jax.shard_map(local_step, mesh=mesh, in_specs=(row_spec, row_spec, row_spec, row_spec, row_spec, P(), row_spec), out_specs=(row_spec, row_spec, row_spec), check_vma=False)
```

```python
import functools

import jax
import jax.numpy as jnp
from jax import lax
from jax.experimental import pallas as pl
from jax.experimental.pallas import tpu as pltpu
from jax.sharding import PartitionSpec as P

F32 = jnp.float32
BF16 = jnp.bfloat16
ROW_CAP = 5
POOL_CHUNK = 16
HOT_CAP = 64
PLANES = 4
HOT_PART = 4
HOT_IN = PLANES * HOT_PART
NEAR_ROW, RELAY_ROW, CROSS_ROW, HOT_ROW, LEVEL_ROW, POS_ROW, PLAN_ROWS = 0, 16, 32, 33, 35, 36, 40
COUNT_LANE = 128
MESH = pl.DeviceIdType.MESH
ORDER = (14, 8, 4, 6, 12, 10, 2, 15, 9, 5, 7, 13, 11, 3, 1)
LEVELS = ((8, 58, 10), (8, 64, 10), (12, 80, 16))


def any_spec():
    return pl.BlockSpec(memory_space=pl.ANY)


def smem_spec():
    return pl.BlockSpec(memory_space=pltpu.SMEM)


def vmem_spec():
    return pl.BlockSpec(memory_space=pltpu.VMEM)


def dot_nn(a, b):
    return jnp.dot(a.astype(BF16), b.astype(BF16), preferred_element_type=F32)


def flag(cond):
    return jnp.where(cond, 1.0, 0.0)


def iota(shape, dim):
    return lax.broadcasted_iota(jnp.int32, shape, dim)


def permutation(n, src_of_row):
    return flag(src_of_row(iota((n, n), 0)) == iota((n, n), 1)).astype(BF16)


def plan_kernel(cfg, table, out, want_s, key_s, hot_s, count_s, union_s):
    n_dev, n_half, per_dev, pair_cap, far_cap, far_base, levels = cfg
    n_cols = n_dev // PLANES
    n_entry = table.shape[1]
    me = lax.axis_index('pool')
    half, in_half = me // n_half, lax.rem(me, n_half)
    partner = (1 - half) * n_half + in_half
    plane, col = me // n_cols, lax.rem(me, n_cols)
    tri = flag(iota((per_dev, per_dev), 0) < iota((per_dev, per_dev), 1)).astype(BF16)
    rowsum = lambda x: jnp.sum(x, axis=1, keepdims=True)

    def hot_entries(dest):
        row = table[pl.ds(dest, 1), :]
        owner = row // per_dev
        return (flag(iota((n_dev, n_entry), 0) == owner).astype(BF16),
                flag(iota((per_dev, n_entry), 0) == row - owner * per_dev).astype(BF16))

    def find(dest, popular):
        by_owner, by_block = hot_entries(dest)
        hits = lax.dot_general(by_owner, by_block, (((1,), (1,)), ((), ())), preferred_element_type=F32)
        want = flag(hits > 0)
        want_s[dest] = want
        return popular + want
    popular = lax.fori_loop(0, n_dev, find, jnp.zeros((n_dev, per_dev), F32))

    def search(_, bounds):
        low, high = bounds
        mid = (low + high) // 2
        fits = jnp.sum(flag(popular >= mid.astype(F32))) <= HOT_CAP
        return jnp.where(fits, low, mid + 1), jnp.where(fits, mid, high)
    steps = n_dev.bit_length()
    threshold, _ = lax.fori_loop(0, steps, search, (jnp.int32(2), jnp.int32(n_dev + 1)))
    hot = flag(popular >= threshold.astype(F32))
    hot_rank = dot_nn(hot, tri)
    hot = hot * flag(hot_rank < 2 * HOT_PART)
    hot_half = jnp.floor(hot_rank * 0.5)
    hot_part = hot_rank - 2 * hot_half
    hot_of = [hot * flag(hot_part == p) for p in range(2)]
    for p in range(2):
        hot_s[p] = hot_of[p]
    hot_s[2] = hot_half

    def rank_rest(dest, carry):
        union, pair_max, far_max = carry
        want = want_s[dest]
        rest = want * (1 - hot)
        key_s[dest] = jnp.where(rest > 0, dot_nn(rest, tri), -1.0)
        num = rowsum(rest)
        count_s[dest] = jnp.broadcast_to(num, (n_dev, 128))
        held = []
        for p in range(2):
            per_owner = rowsum(want * hot_of[p])
            held.append(sum(per_owner[q * n_cols:(q + 1) * n_cols] for q in range(PLANES)))
        across = jnp.where(dest < n_half, num[n_half:], num[:n_half])
        far = across + jnp.concatenate(held, axis=0)
        return jnp.maximum(union, rest), jnp.maximum(pair_max, num), jnp.maximum(far_max, far)

    def rank_half(first, maxima):
        zero = jnp.zeros((n_dev, per_dev), F32)
        return lax.fori_loop(first, first + n_half, rank_rest, (zero,) + maxima)
    union0, pair_max, far_max = rank_half(0, (jnp.zeros((n_dev, 1), F32), jnp.zeros((n_half, 1), F32)))
    union1, pair_max, far_max = rank_half(n_half, (pair_max, far_max))
    for h, union in enumerate((union0, union1)):
        union_s[h] = jnp.where(union > 0, dot_nn(union, tri), -1.0)
    union_max = jnp.maximum(jnp.max(rowsum(union0)[n_half:]), jnp.max(rowsum(union1)[:n_half]))
    pair_max, far_max = jnp.max(pair_max), jnp.max(far_max)
    level = jnp.int32(0)
    for near_send, n_cross, far_send in levels:
        over = (pair_max > near_send) | (union_max > n_cross) | (far_max > far_send)
        level = level + over.astype(jnp.int32)
    out[LEVEL_ROW:LEVEL_ROW + 1, :] = jnp.full((1, per_dev), level, jnp.int32)

    def compact(keys, values, size):
        place = iota((per_dev, size), 1).astype(F32)
        total = 0
        for key, value in zip(keys, values):
            total = total + jnp.sum(jnp.where(key == place, value, 0.0), axis=0, keepdims=True)
        return total

    def put(row, ids, num):
        out[row:row + 1, 0:ids.shape[1]] = ids.astype(jnp.int32)
        if ids.shape[1] < per_dev:
            out[row:row + 1, COUNT_LANE:] = jnp.broadcast_to(num, (1, per_dev - COUNT_LANE)).astype(jnp.int32)

    ids = iota((per_dev, 1), 0).astype(F32)
    dests = [half * n_half + d for d in range(n_half)]
    stack = lambda ref, at: jnp.concatenate([ref[d, pl.ds(at, 1), :] for d in dests], axis=0)
    near_keys = stack(key_s, me)
    relay_keys = [stack(key_s, partner)]
    relay_num = [rowsum(flag(relay_keys[0] >= 0))]
    mine = lax.rem(plane, 2)
    for q in range(PLANES):
        here = stack(want_s, q * n_cols + col) * hot_s[mine, pl.ds(q * n_cols + col, 1), :]
        before = sum(relay_num)
        relay_keys.append(jnp.where(here > 0, dot_nn(here, tri) + before, -1.0))
        relay_num.append(rowsum(here))
    relay_at = [HOT_IN + union_s[half, pl.ds(partner, 1), :]]
    for q in range(PLANES):
        relay_at.append(q * HOT_PART + hot_s[2, pl.ds(q * n_cols + col, 1), :])
    cross_key = union_s[1 - half, pl.ds(me, 1), :]
    hot_keys = [jnp.where(hot_s[p, pl.ds(me, 1), :] > 0, hot_s[2, pl.ds(me, 1), :], -1.0) for p in range(2)]
    rows = [near_keys] + relay_keys + relay_at + [cross_key] + hot_keys
    used = sum(r.shape[0] for r in rows)
    turned = jnp.concatenate(rows + [jnp.zeros((128 - used, per_dev), F32)], axis=0).T
    column = lambda i: turned[:, i:i + 1]
    at0 = n_half * (PLANES + 2)
    values = [column(at0 + q) for q in range(PLANES + 1)]
    near_num = rowsum(flag(near_keys >= 0))
    for d in range(n_half):
        put(NEAR_ROW + d, compact([column(d)], [ids], 128), near_num[d:d + 1])
        keys = [column(n_half * (q + 1) + d) for q in range(PLANES + 1)]
        put(RELAY_ROW + d, compact(keys, values, 128), sum(relay_num)[d:d + 1])
    last = at0 + PLANES + 1
    put(CROSS_ROW, compact([column(last)], [ids], per_dev), None)
    for p in range(2):
        put(HOT_ROW + p, compact([column(last + 1 + p)], [ids], 128), rowsum(flag(hot_keys[p] >= 0)))
    cross_num = rowsum(flag(cross_key >= 0)).astype(jnp.int32)
    out[LEVEL_ROW:LEVEL_ROW + 1, COUNT_LANE:] = jnp.broadcast_to(cross_num, (1, per_dev - COUNT_LANE))

    owner = iota((n_dev, 1), 0)
    group = lax.rem(owner, n_half).astype(F32)
    is_near = owner // n_half == half
    rest_at = jnp.where(is_near, group * pair_cap, far_base + group * far_cap) + key_s[me]
    num = count_s[me, :, 0:1]
    across = jnp.where(half == 0, num[n_half:], num[:n_half])
    place = rest_at
    for p in range(2):
        here = want_s[me] * hot_of[p]
        per_owner = rowsum(here)
        parts = [per_owner[q * n_cols:(q + 1) * n_cols] for q in range(PLANES)]
        holder = p * n_cols + iota((n_cols, 1), 0)
        start = far_base + holder.astype(F32) * far_cap + across[p * n_cols:(p + 1) * n_cols]
        starts = [start]
        for part in parts[:-1]:
            starts.append(starts[-1] + part)
        place = jnp.where(here > 0, jnp.concatenate(starts, axis=0) + dot_nn(here, tri), place)
    place = jnp.maximum(place, 0.0)
    high = jnp.floor(place * (1.0 / 256))
    by_owner, by_block = hot_entries(me)
    picked = dot_nn(high, by_block) * 256 + dot_nn(place - high * 256, by_block)
    pos = jnp.sum(picked * by_owner.astype(F32), axis=0, keepdims=True).astype(jnp.int32)
    for i in range(n_entry // per_dev):
        out[POS_ROW + i:POS_ROW + i + 1, :] = pos[:, i * per_dev:(i + 1) * per_dev]


def pack_pool_kernel(cfg, plan, k_pool, v_pool, x_near, x_cross, x_hot, raw, head_major, in_sem, out_sem):
    per_dev, n_half, pair_cap, block_len, kv_heads = cfg
    n_chunk = per_dev // POOL_CHUNK
    perm = permutation(block_len * kv_heads, lambda r: lax.rem(r, block_len) * kv_heads + r // block_len)

    def chunk_copies(chunk, slot):
        rows = pl.ds(chunk * POOL_CHUNK, POOL_CHUNK)
        return (pltpu.make_async_copy(k_pool.at[rows], raw.at[slot, 0], in_sem.at[slot, 0]),
                pltpu.make_async_copy(v_pool.at[rows], raw.at[slot, 1], in_sem.at[slot, 1]))

    for copy in chunk_copies(0, 0):
        copy.start()

    def turn_chunk(chunk, carry):
        slot = lax.rem(chunk, 2)

        @pl.when(chunk + 1 < n_chunk)
        def _():
            for copy in chunk_copies(chunk + 1, 1 - slot):
                copy.start()

        for copy in chunk_copies(chunk, slot):
            copy.wait()
        for j in range(POOL_CHUNK):
            both = jnp.concatenate([raw[slot, 0, j], raw[slot, 1, j]], axis=1)
            turned = jnp.dot(perm, both, preferred_element_type=F32).astype(BF16)
            head_major[chunk * POOL_CHUNK + j, 0:128, :] = turned[:, 0:128]
            head_major[chunk * POOL_CHUNK + j, 128:256, :] = turned[:, 128:256]
        return carry

    lax.fori_loop(0, n_chunk, turn_chunk, 0)

    def start_list(row, count, dest, base):
        def body(k, carry):
            pltpu.make_async_copy(head_major.at[plan[row, k]], dest.at[base + k], out_sem).start()
            return carry
        lax.fori_loop(0, count, body, 0)

    total = plan[LEVEL_ROW, COUNT_LANE]
    start_list(CROSS_ROW, total, x_cross, 0)
    for q in range(2):
        num = plan[HOT_ROW + q, COUNT_LANE]
        start_list(HOT_ROW + q, num, x_hot, q * HOT_PART)
        total = total + num
    for q in range(n_half):
        num = plan[NEAR_ROW + q, COUNT_LANE]
        start_list(NEAR_ROW + q, num, x_near, q * pair_cap)
        total = total + num

    def drain(k, carry):
        pltpu.make_async_copy(head_major.at[0], x_near.at[0], out_sem).wait()
        return carry
    lax.fori_loop(0, total, drain, 0)


def pack_relay_kernel(cfg, plan, arrived, x_out, stage, in_sem, out_sem):
    n_half, far_cap, n_arrived = cfg

    whole = pltpu.make_async_copy(arrived, stage, in_sem)
    whole.start()
    whole.wait()
    total = 0
    for q in range(n_half):
        def store(k, carry, q=q):
            pltpu.make_async_copy(stage.at[plan[RELAY_ROW + q, k]], x_out.at[q * far_cap + k], out_sem).start()
            return carry
        num = plan[RELAY_ROW + q, COUNT_LANE]
        lax.fori_loop(0, num, store, 0)
        total = total + num

    def drain(k, carry):
        pltpu.make_async_copy(stage.at[0], x_out.at[0], out_sem).wait()
        return carry
    lax.fori_loop(0, total, drain, 0)


def xor_bits(index, bits):
    out = index
    bit = 1
    while bit <= bits:
        if bits & bit:
            out = out + bit - 2 * bit * lax.rem(index // bit, 2)
        bit *= 2
    return out


def exchange_kernel(cfg, *refs):
    n_half, slot_cap, pair_send, n_cross, base = cfg
    first = n_cross > 0
    if first:
        x_pair, x_cross, x_hot, recv, arrived, own, send_sem, recv_sem, own_sem = refs
    else:
        x_pair, _, recv, own, send_sem, recv_sem, own_sem = refs
    me = lax.axis_index('pool')
    in_half = lax.rem(me, n_half)
    half = me // n_half
    n_cols = 2 * n_half // PLANES
    plane, col = me // n_cols, lax.rem(me, n_cols)
    own_group = recv.at[pl.ds(base + in_half * slot_cap, pair_send)]
    sends = []
    for j in ORDER:
        sends.append((half * n_half + xor_bits(in_half, j),
                      x_pair.at[pl.ds(xor_bits(in_half, j) * slot_cap, pair_send)], own_group))
    own_copies = [(x_pair.at[pl.ds(in_half * slot_cap, pair_send)], own.at[pl.ds(0, pair_send)], own_group)]
    if first:
        hot_here = arrived.at[pl.ds(plane * HOT_PART, HOT_PART)]
        hot_for = lambda p: x_hot.at[pl.ds(lax.rem(p, 2) * HOT_PART, HOT_PART)]
        sends.append(((1 - half) * n_half + in_half, x_cross.at[pl.ds(0, n_cross)],
                      arrived.at[pl.ds(HOT_IN, n_cross)]))
        for j in range(1, PLANES):
            to = xor_bits(plane, j)
            sends.append((to * n_cols + col, hot_for(to), hot_here))
        own_copies.append((hot_for(plane), own.at[pl.ds(pair_send, HOT_PART)], hot_here))

    barrier = pltpu.get_barrier_semaphore()
    for peer, _, _ in sends:
        pl.semaphore_signal(barrier, inc=1, device_id=(peer,), device_id_type=MESH)
    own_in = [pltpu.make_async_copy(src, mid, own_sem.at[0, i]) for i, (src, mid, _) in enumerate(own_copies)]
    for copy in own_in:
        copy.start()
    pl.semaphore_wait(barrier, len(sends))
    copies = []
    for i, (peer, src, dst) in enumerate(sends):
        copies.append(pltpu.make_async_remote_copy(
            src_ref=src, dst_ref=dst, send_sem=send_sem.at[i], recv_sem=recv_sem.at[i],
            device_id=(peer,), device_id_type=MESH))
        copies[-1].start()
    for copy in own_in:
        copy.wait()
    own_out = [pltpu.make_async_copy(mid, dst, own_sem.at[1, i]) for i, (_, mid, dst) in enumerate(own_copies)]
    for copy in own_out:
        copy.start()
    for copy in own_out + copies:
        copy.wait()


def attend_kernel(cfg, plan, targets, q_ref, kn_ref, vn_ref, recv, k_pool, v_pool, k_new, v_new,
                  out_ref, k_out, v_out, kv, q_heads, heads_out, sem, pool_buf, new_buf, pool_in, pool_done, new_sem):
    n_pref, block_len, kv_heads, groups, chunk_len, head_dim, n_req, per_dev, n_new = cfg
    req = pl.program_id(0)
    slot = lax.rem(req, 2)
    exp_scale = float(head_dim ** -0.5 * 1.4426950408889634)
    piece = 2 * per_dev // n_req
    per_row = per_dev // n_pref

    def fetch(which, into):
        def body(k, carry):
            pltpu.make_async_copy(recv.at[plan[POS_ROW + which // per_row, lax.rem(which, per_row) * n_pref + k]], kv.at[into, k], sem.at[into]).start()
            return carry
        lax.fori_loop(0, n_pref, body, 0, unroll=8)

    def pool_copies(step, at):
        rows = pl.ds(step * piece, piece)
        pairs = ((k_pool, k_out), (v_pool, v_out))
        return ([pltpu.make_async_copy(src.at[rows], pool_buf.at[at, i], pool_in.at[at, i])
                 for i, (src, _) in enumerate(pairs)],
                [pltpu.make_async_copy(pool_buf.at[at, i], dst.at[rows], pool_done.at[at, i])
                 for i, (_, dst) in enumerate(pairs)])

    new_in = [pltpu.make_async_copy(src, new_buf.at[i], new_sem.at[i]) for i, src in enumerate((k_new, v_new))]

    def new_out(i, which):
        dst = (k_out, v_out)[which]
        return pltpu.make_async_copy(new_buf.at[which, i], dst.at[targets[i]], new_sem.at[2])

    @pl.when(req == 0)
    def _():
        fetch(0, 0)
        for copy in pool_copies(0, 0)[0] + new_in:
            copy.start()

    @pl.when(req + 1 < n_req)
    def _():
        fetch(req + 1, 1 - slot)

    n_step = n_req // 2
    for step in range(n_step):
        @pl.when(req == step)
        def _(step=step):
            at = step % 2
            ins, outs = pool_copies(step, at)
            for copy in ins:
                copy.wait()
            for copy in outs:
                copy.start()
            if step + 1 < n_step:
                if step > 0:
                    for copy in pool_copies(step - 1, 1 - at)[1]:
                        copy.wait()
                for copy in pool_copies(step + 1, 1 - at)[0]:
                    copy.start()

    @pl.when(req == n_step)
    def _():
        for step in (n_step - 2, n_step - 1):
            for copy in pool_copies(step, step % 2)[1]:
                copy.wait()
        for copy in new_in:
            copy.wait()
        for i in range(n_new):
            new_out(i, 0).start()
            new_out(i, 1).start()

    @pl.when(req == n_req - 1)
    def _():
        for i in range(n_new):
            new_out(i, 0).wait()
            new_out(i, 1).wait()

    pltpu.make_async_copy(recv.at[pl.ds(0, n_pref)], kv.at[slot], sem.at[slot]).wait()

    rows = chunk_len * groups
    token = lax.broadcasted_iota(jnp.int32, (rows, chunk_len), 0) // groups
    causal = lax.broadcasted_iota(jnp.int32, (rows, chunk_len), 1) <= token
    n_keys = n_pref * block_len
    nt = (((1,), (1,)), ((), ()))
    span = 256 // kv_heads
    span_tok = span // groups
    to_heads = permutation(256, lambda r: lax.rem(r // groups, span_tok) * (kv_heads * groups)
                           + r // span * groups + lax.rem(r, groups))
    to_tokens = permutation(256, lambda r: lax.rem(r // groups, kv_heads) * span
                            + r // (kv_heads * groups) * groups + lax.rem(r, groups))
    new_heads = permutation(256, lambda r: lax.rem(r, chunk_len) * kv_heads + r // chunk_len)
    for g in range(rows // span):
        part = jnp.dot(to_heads, q_ref[0, g * 256:(g + 1) * 256, :], preferred_element_type=F32).astype(BF16)
        for h in range(kv_heads):
            q_heads[h, g * span:(g + 1) * span, :] = part[h * span:(h + 1) * span]
    new_kv = jnp.concatenate([kn_ref[0], vn_ref[0]], axis=1)
    new_kv = jnp.dot(new_heads, new_kv, preferred_element_type=F32).astype(BF16)
    for h in range(kv_heads):
        q_h = q_heads[h]
        k_own = new_kv[h * chunk_len:(h + 1) * chunk_len, 0:head_dim]
        v_own = new_kv[h * chunk_len:(h + 1) * chunk_len, head_dim:]
        k_h = kv[slot, :, h * block_len:(h + 1) * block_len, :].reshape(n_keys, head_dim)
        v_at = (kv_heads + h) * block_len
        v_h = kv[slot, :, v_at:v_at + block_len, :].reshape(n_keys, head_dim)
        s_pref = lax.dot_general(q_h, k_h, nt, preferred_element_type=F32)
        s_self = lax.dot_general(q_h, k_own, nt, preferred_element_type=F32)
        s_self = jnp.where(causal, s_self, -jnp.inf)
        row_max = jnp.maximum(jnp.max(s_pref, axis=-1, keepdims=True), jnp.max(s_self, axis=-1, keepdims=True))
        e_pref = jnp.exp2((s_pref - row_max) * exp_scale)
        e_self = jnp.exp2((s_self - row_max) * exp_scale)
        total = jnp.sum(e_pref, axis=-1, keepdims=True) + jnp.sum(e_self, axis=-1, keepdims=True)
        inv = 1.0 / total
        p_pref = (e_pref * inv).astype(BF16)
        p_self = (e_self * inv).astype(BF16)
        acc = jnp.dot(p_pref, v_h, preferred_element_type=F32)
        acc = acc + jnp.dot(p_self, v_own, preferred_element_type=F32)
        heads_out[h] = acc.astype(BF16)
    for g in range(rows // span):
        part = heads_out[:, g * span:(g + 1) * span, :].reshape(256, head_dim)
        out_ref[0, g * 256:(g + 1) * 256, :] = jnp.dot(to_tokens, part, preferred_element_type=F32).astype(BF16)


def solution(mesh):
    n_dev = mesh.shape['pool']

    def local_step(queries, k_new, v_new, k_pool, v_pool, block_table, write_ids):
        req_count, chunk_len, q_heads, head_dim = queries.shape
        kv_heads = k_new.shape[2]
        groups = q_heads // kv_heads
        per_dev, block_len = k_pool.shape[0], k_pool.shape[1]
        n_pref = block_table.shape[1]
        block_rows = block_len * kv_heads
        pair_cap = req_count * ROW_CAP
        n_half = n_dev // 2
        n_cols = n_dev // PLANES
        far_cap = pair_cap + HOT_IN
        far_base = n_half * pair_cap
        n_recv = far_base + n_half * far_cap
        plan = pl.pallas_call(
            functools.partial(plan_kernel, (n_dev, n_half, per_dev, pair_cap, far_cap, far_base, LEVELS)),
            out_shape=jax.ShapeDtypeStruct((PLAN_ROWS, per_dev), jnp.int32),
            in_specs=[vmem_spec()], out_specs=vmem_spec(),
            scratch_shapes=[
                pltpu.VMEM((n_dev, n_dev, per_dev), F32),
                pltpu.VMEM((n_dev, n_dev, per_dev), F32),
                pltpu.VMEM((3, n_dev, per_dev), F32),
                pltpu.VMEM((n_dev, n_dev, 128), F32),
                pltpu.VMEM((2, n_dev, per_dev), F32),
            ],
            compiler_params=pltpu.CompilerParams(vmem_limit_bytes=24 << 20),
            name='plan',
        )(block_table.reshape(n_dev, req_count * n_pref))

        block_shape = (2 * block_rows, head_dim)
        shaped = lambda n: jax.ShapeDtypeStruct((n,) + block_shape, BF16)
        flat_pool = (per_dev, block_rows, head_dim)
        k_flat, v_flat = k_pool.reshape(flat_pool), v_pool.reshape(flat_pool)
        x_near, x_cross, x_hot = pl.pallas_call(
            functools.partial(pack_pool_kernel, (per_dev, n_half, pair_cap, block_len, kv_heads)),
            out_shape=(shaped(n_half * pair_cap), shaped(per_dev), shaped(2 * HOT_PART)),
            in_specs=[smem_spec()] + [any_spec()] * 2,
            out_specs=(any_spec(),) * 3,
            scratch_shapes=[
                pltpu.VMEM((2, 2, POOL_CHUNK, block_rows, head_dim), BF16),
                pltpu.VMEM((per_dev,) + block_shape, BF16),
                pltpu.SemaphoreType.DMA((2, 2)),
                pltpu.SemaphoreType.DMA,
            ],
            compiler_params=pltpu.CompilerParams(vmem_limit_bytes=40 << 20),
            name='pack_pool',
        )(plan, k_flat, v_flat)

        rows = chunk_len * groups
        def exchange(level, near_send, n_cross, far_send, x_near, x_cross, x_hot, plan):
            n_arrived = HOT_IN + n_cross

            def exchange_call(first, send, out_shape, n_in, alias, name):
                n_copy = n_half + PLANES
                return pl.pallas_call(
                    functools.partial(exchange_kernel, (
                        n_half, pair_cap if first else far_cap, send, n_cross if first else 0,
                        0 if first else far_base)),
                    out_shape=out_shape, in_specs=[any_spec()] * n_in,
                    out_specs=(any_spec(),) * 2 if first else any_spec(),
                    scratch_shapes=[
                        pltpu.VMEM((send + HOT_PART,) + block_shape, BF16), pltpu.SemaphoreType.DMA((n_copy,)),
                        pltpu.SemaphoreType.DMA((n_copy,)), pltpu.SemaphoreType.DMA((2, 2))],
                    input_output_aliases=alias,
                    compiler_params=pltpu.CompilerParams(
                        collective_id=2 * level + (0 if first else 1), has_side_effects=True,
                        vmem_limit_bytes=8 << 20),
                    name=name)

            recv, arrived = exchange_call(True, near_send, (shaped(n_recv), shaped(n_arrived)), 3, {},
                                          'exchange_near')(x_near, x_cross, x_hot)
            x_relay = pl.pallas_call(
                functools.partial(pack_relay_kernel, (n_half, far_cap, n_arrived)),
                out_shape=shaped(n_half * far_cap),
                in_specs=[smem_spec(), any_spec()], out_specs=any_spec(),
                scratch_shapes=[pltpu.VMEM((n_arrived,) + block_shape, BF16), pltpu.SemaphoreType.DMA,
                                pltpu.SemaphoreType.DMA],
                compiler_params=pltpu.CompilerParams(vmem_limit_bytes=24 << 20), name='pack_relay',
            )(plan, arrived)
            return exchange_call(False, far_send, shaped(n_recv), 2, {1: 0}, 'exchange_far')(x_relay, recv)

        sizes = tuple(LEVELS) + ((pair_cap, per_dev, far_cap),)
        recv = lax.switch(plan[LEVEL_ROW, 0], [functools.partial(exchange, i, *s) for i, s in enumerate(sizes)],
                          x_near, x_cross, x_hot, plan)

        cfg = (n_pref, block_len, kv_heads, groups, chunk_len, head_dim, req_count, per_dev, write_ids.size)
        new_shape = (write_ids.size, block_rows, head_dim)
        row_block = lambda *dims: pl.BlockSpec((1,) + dims, lambda r: (r,) + (0,) * len(dims))
        attn, k_pool_out, v_pool_out = pl.pallas_call(
            functools.partial(attend_kernel, cfg),
            out_shape=(jax.ShapeDtypeStruct((req_count, chunk_len * q_heads, head_dim), BF16),
                       jax.ShapeDtypeStruct(flat_pool, BF16), jax.ShapeDtypeStruct(flat_pool, BF16)),
            grid=(req_count,),
            in_specs=[
                smem_spec(), smem_spec(), row_block(chunk_len * q_heads, head_dim),
                row_block(chunk_len * kv_heads, head_dim), row_block(chunk_len * kv_heads, head_dim),
            ] + [any_spec()] * 5,
            out_specs=(row_block(chunk_len * q_heads, head_dim), any_spec(), any_spec()),
            scratch_shapes=[
                pltpu.VMEM((2, n_pref) + block_shape, BF16),
                pltpu.VMEM((kv_heads, rows, head_dim), BF16),
                pltpu.VMEM((kv_heads, rows, head_dim), BF16),
                pltpu.SemaphoreType.DMA((2,)),
                pltpu.VMEM((2, 2, 2 * per_dev // req_count, block_rows, head_dim), BF16),
                pltpu.VMEM((2,) + new_shape, BF16),
                pltpu.SemaphoreType.DMA((2, 2)),
                pltpu.SemaphoreType.DMA((2, 2)),
                pltpu.SemaphoreType.DMA((3,)),
            ],
            compiler_params=pltpu.CompilerParams(
                vmem_limit_bytes=56 << 20, dimension_semantics=('arbitrary',)),
            name='attend',
        )(plan, write_ids.reshape(-1), queries.reshape(req_count, chunk_len * q_heads, head_dim),
          k_new.reshape(req_count, chunk_len * kv_heads, head_dim),
          v_new.reshape(req_count, chunk_len * kv_heads, head_dim), recv, k_flat, v_flat,
          k_new.reshape(new_shape), v_new.reshape(new_shape))
        attn_out = attn.reshape(req_count, chunk_len, q_heads, head_dim)
        return attn_out, k_pool_out.reshape(k_pool.shape), v_pool_out.reshape(v_pool.shape)

    row_spec = P('pool')
    return jax.shard_map(local_step, mesh=mesh, in_specs=(row_spec, row_spec, row_spec, row_spec, row_spec, P(), row_spec), out_specs=(row_spec, row_spec, row_spec), check_vma=False)
```

```python
import functools

import jax
import jax.numpy as jnp
from jax import lax
from jax.experimental import pallas as pl
from jax.experimental.pallas import tpu as pltpu
from jax.sharding import PartitionSpec as P

F32 = jnp.float32
BF16 = jnp.bfloat16
ROW_CAP = 5
FIND_STEP = 4
PIECE = 32
HOT_CAP = 64
PLANES = 4
HOT_PART = 4
HOT_IN = PLANES * HOT_PART
NEAR_ROW, RELAY_ROW, CROSS_ROW, HOT_ROW, LEVEL_ROW, POS_ROW, PLAN_ROWS = 0, 16, 32, 33, 35, 36, 40
COUNT_LANE = 128
LIST_LANES = 64
MESH = pl.DeviceIdType.MESH
ORDER = (14, 8, 4, 6, 12, 10, 2, 15, 9, 5, 7, 13, 11, 3, 1)
LEVELS = ((8, 58, 10), (8, 64, 10), (12, 80, 16))


def any_spec():
    return pl.BlockSpec(memory_space=pl.ANY)


def smem_spec():
    return pl.BlockSpec(memory_space=pltpu.SMEM)


def vmem_spec():
    return pl.BlockSpec(memory_space=pltpu.VMEM)


def dot_nn(a, b):
    return jnp.dot(a.astype(BF16), b.astype(BF16), preferred_element_type=F32)


def flag(cond):
    return jnp.where(cond, 1.0, 0.0)


def iota(shape, dim):
    return lax.broadcasted_iota(jnp.int32, shape, dim)


def permutation(n, src_of_row):
    return flag(src_of_row(iota((n, n), 0)) == iota((n, n), 1)).astype(BF16)


def plan_kernel(cfg, table, k_pool, v_pool, out, x_near, x_cross, x_hot,
                want_s, key_s, hot_s, count_s, union_s, raw, head_major, plan, in_sem, plan_sem, out_sem):
    n_dev, n_half, per_dev, pair_cap, far_cap, far_base, block_len, kv_heads, levels = cfg
    n_group = n_dev // FIND_STEP
    group_blocks = per_dev // n_group
    perm = permutation(block_len * kv_heads, lambda r: lax.rem(r, block_len) * kv_heads + r // block_len)

    def group_copies(group):
        rows = pl.ds(group * group_blocks, group_blocks)
        return [pltpu.make_async_copy(src.at[rows], raw.at[i, rows], in_sem.at[i, group])
                for i, src in enumerate((k_pool, v_pool))]

    for group in range(n_group):
        for copy in group_copies(group):
            copy.start()
    n_cols = n_dev // PLANES
    n_entry = table.shape[1]
    me = lax.axis_index('pool')
    half, in_half = me // n_half, lax.rem(me, n_half)
    partner = (1 - half) * n_half + in_half
    plane, col = me // n_cols, lax.rem(me, n_cols)
    tri = flag(iota((per_dev, per_dev), 0) < iota((per_dev, per_dev), 1)).astype(BF16)
    rowsum = lambda x: jnp.sum(x, axis=1, keepdims=True)

    def hot_entries(dest):
        row = table[pl.ds(dest, 1), :]
        owner = row // per_dev
        return (flag(iota((n_dev, n_entry), 0) == owner).astype(BF16),
                flag(iota((per_dev, n_entry), 0) == row - owner * per_dev).astype(BF16))

    def find(dest, popular):
        by_owner, by_block = hot_entries(dest)
        hits = lax.dot_general(by_owner, by_block, (((1,), (1,)), ((), ())), preferred_element_type=F32)
        want = flag(hits > 0)
        want_s[dest] = want
        return popular + want

    def find_and_turn(group, popular):
        for copy in group_copies(group):
            copy.wait()
        for i in range(FIND_STEP):
            popular = find(group * FIND_STEP + i, popular)
            for j in range(group_blocks // FIND_STEP):
                block = group * group_blocks + i * (group_blocks // FIND_STEP) + j
                turned = dot_nn(perm, jnp.concatenate([raw[0, block], raw[1, block]], axis=1)).astype(BF16)
                head_major[block, 0:128, :] = turned[:, 0:128]
                head_major[block, 128:256, :] = turned[:, 128:256]
        return popular
    popular = lax.fori_loop(0, n_group, find_and_turn, jnp.zeros((n_dev, per_dev), F32))

    def search(_, bounds):
        low, high = bounds
        mid = (low + high) // 2
        fits = jnp.sum(flag(popular >= mid.astype(F32))) <= HOT_CAP
        return jnp.where(fits, low, mid + 1), jnp.where(fits, mid, high)
    steps = n_dev.bit_length()
    threshold, _ = lax.fori_loop(0, steps, search, (jnp.int32(2), jnp.int32(n_dev + 1)))
    hot = flag(popular >= threshold.astype(F32))
    hot_rank = dot_nn(hot, tri)
    hot = hot * flag(hot_rank < 2 * HOT_PART)
    hot_half = jnp.floor(hot_rank * 0.5)
    hot_part = hot_rank - 2 * hot_half
    hot_of = [hot * flag(hot_part == p) for p in range(2)]
    for p in range(2):
        hot_s[p] = hot_of[p]
    hot_s[2] = hot_half

    def rank_rest(dest, carry):
        union, pair_max, far_max = carry
        want = want_s[dest]
        rest = want * (1 - hot)
        key_s[dest] = jnp.where(rest > 0, dot_nn(rest, tri), -1.0)
        num = rowsum(rest)
        count_s[dest] = jnp.broadcast_to(num, (n_dev, 128))
        held = []
        for p in range(2):
            per_owner = rowsum(want * hot_of[p])
            held.append(sum(per_owner[q * n_cols:(q + 1) * n_cols] for q in range(PLANES)))
        across = jnp.where(dest < n_half, num[n_half:], num[:n_half])
        far = across + jnp.concatenate(held, axis=0)
        return jnp.maximum(union, rest), jnp.maximum(pair_max, num), jnp.maximum(far_max, far)

    def rank_half(first, maxima):
        zero = jnp.zeros((n_dev, per_dev), F32)

        def several(step, carry):
            for i in range(FIND_STEP):
                carry = rank_rest(first + step * FIND_STEP + i, carry)
            return carry
        return lax.fori_loop(0, n_half // FIND_STEP, several, (zero,) + maxima)
    union0, pair_max, far_max = rank_half(0, (jnp.zeros((n_dev, 1), F32), jnp.zeros((n_half, 1), F32)))
    union1, pair_max, far_max = rank_half(n_half, (pair_max, far_max))
    for h, union in enumerate((union0, union1)):
        union_s[h] = jnp.where(union > 0, dot_nn(union, tri), -1.0)
    union_max = jnp.maximum(jnp.max(rowsum(union0)[n_half:]), jnp.max(rowsum(union1)[:n_half]))
    pair_max, far_max = jnp.max(pair_max), jnp.max(far_max)
    level = jnp.int32(0)
    for near_send, n_cross, far_send in levels:
        over = (pair_max > near_send) | (union_max > n_cross) | (far_max > far_send)
        level = level + over.astype(jnp.int32)
    out[LEVEL_ROW:LEVEL_ROW + 1, :] = jnp.full((1, per_dev), level, jnp.int32)

    def compact(keys, values, size):
        places = iota((size, per_dev), 0).astype(F32)
        hits = jnp.concatenate([flag(key == places).astype(BF16) for key in keys], axis=1)
        values = jnp.broadcast_to(jnp.concatenate(values, axis=1), (8, per_dev * len(keys))).astype(BF16)
        ids = lax.dot_general(values, hits, (((1,), (1,)), ((), ())), preferred_element_type=F32)
        return ids[0:1]

    def put(row, ids, num):
        out[row:row + 1, 0:ids.shape[1]] = ids.astype(jnp.int32)
        if ids.shape[1] < per_dev:
            out[row:row + 1, COUNT_LANE:] = jnp.broadcast_to(num, (1, per_dev - COUNT_LANE)).astype(jnp.int32)

    ids = iota((1, per_dev), 1).astype(F32)
    dests = [half * n_half + d for d in range(n_half)]
    stack = lambda ref, at: jnp.concatenate([ref[d, pl.ds(at, 1), :] for d in dests], axis=0)
    near_keys = stack(key_s, me)
    relay_keys = [stack(key_s, partner)]
    relay_num = [rowsum(flag(relay_keys[0] >= 0))]
    mine = lax.rem(plane, 2)
    for q in range(PLANES):
        here = stack(want_s, q * n_cols + col) * hot_s[mine, pl.ds(q * n_cols + col, 1), :]
        before = sum(relay_num)
        relay_keys.append(jnp.where(here > 0, dot_nn(here, tri) + before, -1.0))
        relay_num.append(rowsum(here))
    relay_at = [union_s[half, pl.ds(partner, 1), :]]
    for q in range(PLANES):
        relay_at.append(q * HOT_PART + hot_s[2, pl.ds(q * n_cols + col, 1), :])
    cross_key = union_s[1 - half, pl.ds(me, 1), :]
    hot_keys = [jnp.where(hot_s[p, pl.ds(me, 1), :] > 0, hot_s[2, pl.ds(me, 1), :], -1.0) for p in range(2)]
    near_num = rowsum(flag(near_keys >= 0))
    for d in range(n_half):
        put(NEAR_ROW + d, compact([near_keys[d:d + 1]], [ids], LIST_LANES), near_num[d:d + 1])
        listed = compact([keys[d:d + 1] for keys in relay_keys], relay_at, LIST_LANES)
        from_partner = flag(iota((1, LIST_LANES), 1).astype(F32) < relay_num[0][d:d + 1])
        put(RELAY_ROW + d, listed + HOT_IN * from_partner, sum(relay_num)[d:d + 1])
    put(CROSS_ROW, compact([cross_key], [ids], per_dev), None)
    for p in range(2):
        put(HOT_ROW + p, compact([hot_keys[p]], [ids], LIST_LANES), rowsum(flag(hot_keys[p] >= 0)))
    cross_num = rowsum(flag(cross_key >= 0)).astype(jnp.int32)
    out[LEVEL_ROW:LEVEL_ROW + 1, COUNT_LANE:] = jnp.broadcast_to(cross_num, (1, per_dev - COUNT_LANE))

    owner = iota((n_dev, 1), 0)
    group = lax.rem(owner, n_half).astype(F32)
    is_near = owner // n_half == half
    rest_at = jnp.where(is_near, group * pair_cap, far_base + group * far_cap) + key_s[me]
    num = count_s[me, :, 0:1]
    across = jnp.where(half == 0, num[n_half:], num[:n_half])
    place = rest_at
    for p in range(2):
        here = want_s[me] * hot_of[p]
        per_owner = rowsum(here)
        parts = [per_owner[q * n_cols:(q + 1) * n_cols] for q in range(PLANES)]
        holder = p * n_cols + iota((n_cols, 1), 0)
        start = far_base + holder.astype(F32) * far_cap + across[p * n_cols:(p + 1) * n_cols]
        starts = [start]
        for part in parts[:-1]:
            starts.append(starts[-1] + part)
        place = jnp.where(here > 0, jnp.concatenate(starts, axis=0) + dot_nn(here, tri), place)
    place = jnp.maximum(place, 0.0)
    high = jnp.floor(place * (1.0 / 256))
    by_owner, by_block = hot_entries(me)
    picked = dot_nn(high, by_block) * 256 + dot_nn(place - high * 256, by_block)
    pos = jnp.sum(picked * by_owner.astype(F32), axis=0, keepdims=True).astype(jnp.int32)
    for i in range(n_entry // per_dev):
        out[POS_ROW + i:POS_ROW + i + 1, :] = pos[:, i * per_dev:(i + 1) * per_dev]

    to_scalar = pltpu.make_async_copy(out, plan, plan_sem)
    to_scalar.start()
    to_scalar.wait()

    def start_list(row, count, dest, base):
        def body(k, carry):
            pltpu.make_async_copy(head_major.at[plan[row, k]], dest.at[base + k], out_sem).start()
            return carry
        lax.fori_loop(0, count, body, 0)

    total = plan[LEVEL_ROW, COUNT_LANE]
    start_list(CROSS_ROW, total, x_cross, 0)
    for q in range(2):
        count = plan[HOT_ROW + q, COUNT_LANE]
        start_list(HOT_ROW + q, count, x_hot, q * HOT_PART)
        total = total + count
    for q in range(n_half):
        count = plan[NEAR_ROW + q, COUNT_LANE]
        start_list(NEAR_ROW + q, count, x_near, q * pair_cap)
        total = total + count

    def drain(k, carry):
        pltpu.make_async_copy(head_major.at[0], x_near.at[0], out_sem).wait()
        return carry
    lax.fori_loop(0, total, drain, 0)


def pack_relay_kernel(cfg, plan, arrived, x_out, stage, in_sem, out_sem):
    n_half, far_cap, n_arrived = cfg

    whole = pltpu.make_async_copy(arrived, stage, in_sem)
    whole.start()
    whole.wait()
    total = 0
    for q in range(n_half):
        def store(k, carry, q=q):
            pltpu.make_async_copy(stage.at[plan[RELAY_ROW + q, k]], x_out.at[q * far_cap + k], out_sem).start()
            return carry
        num = plan[RELAY_ROW + q, COUNT_LANE]
        lax.fori_loop(0, num, store, 0)
        total = total + num

    def drain(k, carry):
        pltpu.make_async_copy(stage.at[0], x_out.at[0], out_sem).wait()
        return carry
    lax.fori_loop(0, total, drain, 0)


def xor_bits(index, bits):
    out = index
    bit = 1
    while bit <= bits:
        if bits & bit:
            out = out + bit - 2 * bit * lax.rem(index // bit, 2)
        bit *= 2
    return out


def exchange_kernel(cfg, *refs):
    n_half, slot_cap, pair_send, n_cross, base = cfg
    first = n_cross > 0
    if first:
        x_pair, x_cross, x_hot, recv, arrived, own, send_sem, recv_sem, own_sem = refs
    else:
        x_pair, _, recv, own, send_sem, recv_sem, own_sem = refs
    me = lax.axis_index('pool')
    in_half = lax.rem(me, n_half)
    half = me // n_half
    n_cols = 2 * n_half // PLANES
    plane, col = me // n_cols, lax.rem(me, n_cols)
    own_group = recv.at[pl.ds(base + in_half * slot_cap, pair_send)]
    sends = []
    for j in ORDER:
        sends.append((half * n_half + xor_bits(in_half, j),
                      x_pair.at[pl.ds(xor_bits(in_half, j) * slot_cap, pair_send)], own_group))
    own_copies = [(x_pair.at[pl.ds(in_half * slot_cap, pair_send)], own.at[pl.ds(0, pair_send)], own_group)]
    if first:
        hot_here = arrived.at[pl.ds(plane * HOT_PART, HOT_PART)]
        hot_for = lambda p: x_hot.at[pl.ds(lax.rem(p, 2) * HOT_PART, HOT_PART)]
        sends.append(((1 - half) * n_half + in_half, x_cross.at[pl.ds(0, n_cross)],
                      arrived.at[pl.ds(HOT_IN, n_cross)]))
        for j in range(1, PLANES):
            to = xor_bits(plane, j)
            sends.append((to * n_cols + col, hot_for(to), hot_here))
        own_copies.append((hot_for(plane), own.at[pl.ds(pair_send, HOT_PART)], hot_here))

    barrier = pltpu.get_barrier_semaphore()
    for peer, _, _ in sends:
        pl.semaphore_signal(barrier, inc=1, device_id=(peer,), device_id_type=MESH)
    own_in = [pltpu.make_async_copy(src, mid, own_sem.at[0, i]) for i, (src, mid, _) in enumerate(own_copies)]
    for copy in own_in:
        copy.start()
    pl.semaphore_wait(barrier, len(sends))
    copies = []
    for i, (peer, src, dst) in enumerate(sends):
        copies.append(pltpu.make_async_remote_copy(
            src_ref=src, dst_ref=dst, send_sem=send_sem.at[i], recv_sem=recv_sem.at[i],
            device_id=(peer,), device_id_type=MESH))
        copies[-1].start()
    for copy in own_in:
        copy.wait()
    own_out = [pltpu.make_async_copy(mid, dst, own_sem.at[1, i]) for i, (_, mid, dst) in enumerate(own_copies)]
    for copy in own_out:
        copy.start()
    for copy in own_out + copies:
        copy.wait()


def attend_kernel(cfg, plan, targets, q_ref, kn_ref, vn_ref, recv, k_pool, v_pool, k_new, v_new,
                  out_ref, k_out, v_out, kv, q_heads, heads_out, new_heads_kv, s_pref, s_self, p_pref, p_self, sem, pool_buf, new_buf, pool_in, pool_done, new_sem):
    n_pref, block_len, kv_heads, groups, chunk_len, head_dim, n_req, per_dev, n_new = cfg
    req = pl.program_id(0)
    slot = lax.rem(req, 2)
    exp_scale = float(head_dim ** -0.5 * 1.4426950408889634)
    piece = 2 * per_dev // n_req
    per_row = per_dev // n_pref

    def fetch(which, into, first, num):
        row, lane = POS_ROW + which // per_row, lax.rem(which, per_row) * n_pref
        for k in range(num):
            pltpu.make_async_copy(recv.at[plan[row, lane + first + k]], kv.at[into, first + k], sem.at[into]).start()

    def pool_copies(step, at):
        rows = pl.ds(step * piece, piece)
        pairs = ((k_pool, k_out), (v_pool, v_out))
        return ([pltpu.make_async_copy(src.at[rows], pool_buf.at[at, i], pool_in.at[at, i])
                 for i, (src, _) in enumerate(pairs)],
                [pltpu.make_async_copy(pool_buf.at[at, i], dst.at[rows], pool_done.at[at, i])
                 for i, (_, dst) in enumerate(pairs)])

    new_in = [pltpu.make_async_copy(src, new_buf.at[i], new_sem.at[i]) for i, src in enumerate((k_new, v_new))]

    def new_out(i, which):
        dst = (k_out, v_out)[which]
        return pltpu.make_async_copy(new_buf.at[which, i], dst.at[targets[i]], new_sem.at[2])

    @pl.when(req == 0)
    def _():
        fetch(0, 0, 0, n_pref)
        for copy in pool_copies(0, 0)[0] + new_in:
            copy.start()

    n_step = n_req // 2
    for step in range(n_step):
        @pl.when(req == step)
        def _(step=step):
            at = step % 2
            ins, outs = pool_copies(step, at)
            for copy in ins:
                copy.wait()
            for copy in outs:
                copy.start()
            if step + 1 < n_step:
                if step > 0:
                    for copy in pool_copies(step - 1, 1 - at)[1]:
                        copy.wait()
                for copy in pool_copies(step + 1, 1 - at)[0]:
                    copy.start()

    @pl.when(req == n_step)
    def _():
        for step in (n_step - 2, n_step - 1):
            for copy in pool_copies(step, step % 2)[1]:
                copy.wait()
        for copy in new_in:
            copy.wait()
        for i in range(n_new):
            new_out(i, 0).start()
            new_out(i, 1).start()

    @pl.when(req == n_req - 1)
    def _():
        for i in range(n_new):
            new_out(i, 0).wait()
            new_out(i, 1).wait()

    def whole_request(at):
        return pltpu.make_async_copy(recv.at[pl.ds(0, n_pref)], kv.at[at], sem.at[at])

    whole_request(slot).wait()
    aligned = lambda i, n: pl.multiple_of(i * n, n)

    rows = chunk_len * groups
    token = lax.broadcasted_iota(jnp.int32, (rows, chunk_len), 0) // groups
    causal = lax.broadcasted_iota(jnp.int32, (rows, chunk_len), 1) <= token
    n_keys = n_pref * block_len
    nt = (((1,), (1,)), ((), ()))
    span = 256 // kv_heads
    span_tok = span // groups
    to_heads = permutation(256, lambda r: lax.rem(r // groups, span_tok) * (kv_heads * groups)
                           + r // span * groups + lax.rem(r, groups))
    to_tokens = permutation(256, lambda r: lax.rem(r // groups, kv_heads) * span
                            + r // (kv_heads * groups) * groups + lax.rem(r, groups))
    new_heads = permutation(256, lambda r: lax.rem(r, chunk_len) * kv_heads + r // chunk_len)
    for g in range(rows // span):
        part = jnp.dot(to_heads, q_ref[0, g * 256:(g + 1) * 256, :], preferred_element_type=F32).astype(BF16)
        for h in range(kv_heads):
            q_heads[h, g * span:(g + 1) * span, :] = part[h * span:(h + 1) * span]
    new_kv = jnp.concatenate([kn_ref[0], vn_ref[0]], axis=1)
    new_heads_kv[...] = jnp.dot(new_heads, new_kv, preferred_element_type=F32).astype(BF16)
    def scores(h, at):
        k_h = kv[slot, :, pl.ds(aligned(h, block_len), block_len), :].reshape(n_keys, head_dim)
        k_own = new_heads_kv[pl.ds(aligned(h, chunk_len), chunk_len), 0:head_dim]
        s_pref[at] = lax.dot_general(q_heads[h], k_h, nt, preferred_element_type=F32)
        s_own = lax.dot_general(q_heads[h], k_own, nt, preferred_element_type=F32)
        s_self[at] = jnp.where(causal, s_own, -jnp.inf)

    def probabilities(h, at):
        for first in range(0, rows, PIECE):
            part = pl.ds(first, PIECE)
            far, own = s_pref[at, part], s_self[at, part]
            row_max = jnp.maximum(jnp.max(far, axis=-1, keepdims=True), jnp.max(own, axis=-1, keepdims=True))
            far = jnp.exp2((far - row_max) * exp_scale)
            own = jnp.exp2((own - row_max) * exp_scale)
            inv = 1.0 / (jnp.sum(far, axis=-1, keepdims=True) + jnp.sum(own, axis=-1, keepdims=True))
            p_pref[at, part] = (far * inv).astype(BF16)
            p_self[at, part] = (own * inv).astype(BF16)

    def values(h, at):
        v_h = kv[slot, :, pl.ds(aligned(kv_heads + h, block_len), block_len), :].reshape(n_keys, head_dim)
        v_own = new_heads_kv[pl.ds(aligned(h, chunk_len), chunk_len), head_dim:]
        acc = jnp.dot(p_pref[at], v_h, preferred_element_type=F32)
        acc = acc + jnp.dot(p_self[at], v_own, preferred_element_type=F32)
        heads_out[h] = acc.astype(BF16)

    n_part = n_pref // kv_heads
    after = jnp.minimum(req + 1, n_req - 1)

    fetch(after, 1 - slot, 0, n_part)
    scores(0, 0)
    fetch(after, 1 - slot, n_part, n_part)
    scores(1, 1)
    probabilities(0, 0)

    def steady(pair, carry):
        for at in range(2):
            h = 2 * pair + at
            fetch(after, 1 - slot, h * n_part, n_part)
            scores(h, at)
            probabilities(h - 1, 1 - at)
            values(h - 2, at)
        return carry
    lax.fori_loop(1, kv_heads // 2, steady, 0)
    probabilities(kv_heads - 1, 1)
    values(kv_heads - 2, 0)
    values(kv_heads - 1, 1)
    for g in range(rows // span):
        part = heads_out[:, g * span:(g + 1) * span, :].reshape(256, head_dim)
        out_ref[0, g * 256:(g + 1) * 256, :] = jnp.dot(to_tokens, part, preferred_element_type=F32).astype(BF16)

    @pl.when(req == n_req - 1)
    def _():
        whole_request(1 - slot).wait()


def solution(mesh):
    n_dev = mesh.shape['pool']

    def local_step(queries, k_new, v_new, k_pool, v_pool, block_table, write_ids):
        req_count, chunk_len, q_heads, head_dim = queries.shape
        kv_heads = k_new.shape[2]
        groups = q_heads // kv_heads
        per_dev, block_len = k_pool.shape[0], k_pool.shape[1]
        n_pref = block_table.shape[1]
        block_rows = block_len * kv_heads
        pair_cap = req_count * ROW_CAP
        n_half = n_dev // 2
        rows = chunk_len * groups
        n_cols = n_dev // PLANES
        far_cap = pair_cap + HOT_IN
        far_base = n_half * pair_cap
        n_recv = far_base + n_half * far_cap
        block_shape = (2 * block_rows, head_dim)
        shaped = lambda n: jax.ShapeDtypeStruct((n,) + block_shape, BF16)
        flat_pool = (per_dev, block_rows, head_dim)
        k_flat, v_flat = k_pool.reshape(flat_pool), v_pool.reshape(flat_pool)
        plan, x_near, x_cross, x_hot = pl.pallas_call(
            functools.partial(plan_kernel, (n_dev, n_half, per_dev, pair_cap, far_cap, far_base, block_len,
                                            kv_heads, LEVELS)),
            out_shape=(jax.ShapeDtypeStruct((PLAN_ROWS, per_dev), jnp.int32),
                       shaped(n_half * pair_cap), shaped(per_dev), shaped(2 * HOT_PART)),
            in_specs=[vmem_spec()] + [any_spec()] * 2, out_specs=(vmem_spec(),) + (any_spec(),) * 3,
            scratch_shapes=[
                pltpu.VMEM((n_dev, n_dev, per_dev), F32),
                pltpu.VMEM((n_dev, n_dev, per_dev), F32),
                pltpu.VMEM((3, n_dev, per_dev), F32),
                pltpu.VMEM((n_dev, n_dev, 128), F32),
                pltpu.VMEM((2, n_dev, per_dev), F32),
                pltpu.VMEM((2,) + flat_pool, BF16),
                pltpu.VMEM((per_dev,) + block_shape, BF16),
                pltpu.SMEM((PLAN_ROWS, per_dev), jnp.int32),
                pltpu.SemaphoreType.DMA((2, n_dev // FIND_STEP)),
                pltpu.SemaphoreType.DMA,
                pltpu.SemaphoreType.DMA,
            ],
            compiler_params=pltpu.CompilerParams(vmem_limit_bytes=56 << 20),
            name='plan',
        )(block_table.reshape(n_dev, req_count * n_pref), k_flat, v_flat)

        def exchange(level, near_send, n_cross, far_send, x_near, x_cross, x_hot, plan):
            n_arrived = HOT_IN + n_cross

            def exchange_call(first, send, out_shape, n_in, alias, name):
                n_copy = n_half + PLANES
                return pl.pallas_call(
                    functools.partial(exchange_kernel, (
                        n_half, pair_cap if first else far_cap, send, n_cross if first else 0,
                        0 if first else far_base)),
                    out_shape=out_shape, in_specs=[any_spec()] * n_in,
                    out_specs=(any_spec(),) * 2 if first else any_spec(),
                    scratch_shapes=[
                        pltpu.VMEM((send + HOT_PART,) + block_shape, BF16), pltpu.SemaphoreType.DMA((n_copy,)),
                        pltpu.SemaphoreType.DMA((n_copy,)), pltpu.SemaphoreType.DMA((2, 2))],
                    input_output_aliases=alias,
                    compiler_params=pltpu.CompilerParams(
                        collective_id=2 * level + (0 if first else 1), has_side_effects=True,
                        vmem_limit_bytes=8 << 20),
                    name=name)

            recv, arrived = exchange_call(True, near_send, (shaped(n_recv), shaped(n_arrived)), 3, {},
                                          'exchange_near')(x_near, x_cross, x_hot)
            x_relay = pl.pallas_call(
                functools.partial(pack_relay_kernel, (n_half, far_cap, n_arrived)),
                out_shape=shaped(n_half * far_cap),
                in_specs=[smem_spec(), any_spec()], out_specs=any_spec(),
                scratch_shapes=[pltpu.VMEM((n_arrived,) + block_shape, BF16), pltpu.SemaphoreType.DMA,
                                pltpu.SemaphoreType.DMA],
                compiler_params=pltpu.CompilerParams(vmem_limit_bytes=24 << 20), name='pack_relay',
            )(plan, arrived)
            return exchange_call(False, far_send, shaped(n_recv), 2, {1: 0}, 'exchange_far')(x_relay, recv)

        sizes = tuple(LEVELS) + ((pair_cap, per_dev, far_cap),)
        recv = lax.switch(plan[LEVEL_ROW, 0], [functools.partial(exchange, i, *s) for i, s in enumerate(sizes)],
                          x_near, x_cross, x_hot, plan)

        cfg = (n_pref, block_len, kv_heads, groups, chunk_len, head_dim, req_count, per_dev, write_ids.size)
        new_shape = (write_ids.size, block_rows, head_dim)
        row_block = lambda *dims: pl.BlockSpec((1,) + dims, lambda r: (r,) + (0,) * len(dims))
        attn, k_pool_out, v_pool_out = pl.pallas_call(
            functools.partial(attend_kernel, cfg),
            out_shape=(jax.ShapeDtypeStruct((req_count, chunk_len * q_heads, head_dim), BF16),
                       jax.ShapeDtypeStruct(flat_pool, BF16), jax.ShapeDtypeStruct(flat_pool, BF16)),
            grid=(req_count,),
            in_specs=[
                smem_spec(), smem_spec(), row_block(chunk_len * q_heads, head_dim),
                row_block(chunk_len * kv_heads, head_dim), row_block(chunk_len * kv_heads, head_dim),
            ] + [any_spec()] * 5,
            out_specs=(row_block(chunk_len * q_heads, head_dim), any_spec(), any_spec()),
            scratch_shapes=[
                pltpu.VMEM((2, n_pref) + block_shape, BF16),
                pltpu.VMEM((kv_heads, rows, head_dim), BF16),
                pltpu.VMEM((kv_heads, rows, head_dim), BF16),
                pltpu.VMEM((chunk_len * kv_heads, 2 * head_dim), BF16),
                pltpu.VMEM((2, rows, n_pref * block_len), F32),
                pltpu.VMEM((2, rows, chunk_len), F32),
                pltpu.VMEM((2, rows, n_pref * block_len), BF16),
                pltpu.VMEM((2, rows, chunk_len), BF16),
                pltpu.SemaphoreType.DMA((2,)),
                pltpu.VMEM((2, 2, 2 * per_dev // req_count, block_rows, head_dim), BF16),
                pltpu.VMEM((2,) + new_shape, BF16),
                pltpu.SemaphoreType.DMA((2, 2)),
                pltpu.SemaphoreType.DMA((2, 2)),
                pltpu.SemaphoreType.DMA((3,)),
            ],
            compiler_params=pltpu.CompilerParams(
                vmem_limit_bytes=56 << 20, dimension_semantics=('arbitrary',)),
            name='attend',
        )(plan, write_ids.reshape(-1), queries.reshape(req_count, chunk_len * q_heads, head_dim),
          k_new.reshape(req_count, chunk_len * kv_heads, head_dim),
          v_new.reshape(req_count, chunk_len * kv_heads, head_dim), recv, k_flat, v_flat,
          k_new.reshape(new_shape), v_new.reshape(new_shape))
        attn_out = attn.reshape(req_count, chunk_len, q_heads, head_dim)
        return attn_out, k_pool_out.reshape(k_pool.shape), v_pool_out.reshape(v_pool.shape)

    row_spec = P('pool')
    return jax.shard_map(local_step, mesh=mesh, in_specs=(row_spec, row_spec, row_spec, row_spec, row_spec, P(), row_spec), out_specs=(row_spec, row_spec, row_spec), check_vma=False)
```

```python
import functools

import jax
import jax.numpy as jnp
from jax import lax
from jax.experimental import pallas as pl
from jax.experimental.pallas import tpu as pltpu
from jax.sharding import PartitionSpec as P

F32 = jnp.float32
BF16 = jnp.bfloat16
ROW_CAP = 5
FIND_STEP = 4
PIECE = 32
HOT_CAP = 64
PLANES = 4
HOT_PART = 4
HOT_IN = PLANES * HOT_PART
NEAR_ROW, RELAY_ROW, CROSS_ROW, HOT_ROW, LEVEL_ROW, POS_ROW, PLAN_ROWS = 0, 16, 32, 33, 35, 36, 40
COUNT_LANE = 128
LIST_LANES = 64
MESH = pl.DeviceIdType.MESH
ORDER = (14, 8, 4, 6, 12, 10, 2, 15, 9, 5, 7, 13, 11, 3, 1)
LEVELS = ((8, 54, 10), (8, 56, 10), (8, 58, 10), (8, 61, 10), (8, 64, 10), (12, 80, 16))


def any_spec():
    return pl.BlockSpec(memory_space=pl.ANY)


def smem_spec():
    return pl.BlockSpec(memory_space=pltpu.SMEM)


def vmem_spec():
    return pl.BlockSpec(memory_space=pltpu.VMEM)


def dot_nn(a, b):
    return jnp.dot(a.astype(BF16), b.astype(BF16), preferred_element_type=F32)


def flag(cond):
    return jnp.where(cond, 1.0, 0.0)


def iota(shape, dim):
    return lax.broadcasted_iota(jnp.int32, shape, dim)


def permutation(n, src_of_row):
    return flag(src_of_row(iota((n, n), 0)) == iota((n, n), 1)).astype(BF16)


def plan_kernel(cfg, targets, table_in, k_pool, v_pool, k_new, v_new, out, x_near, x_cross, x_hot, k_out, v_out,
                by_row, table, want_s, key_s, hot_s, count_s, union_s, raw, head_major, plan, new_buf,
                in_sem, pool_sem, new_sem, plan_sem, out_sem):
    n_dev, n_half, per_dev, pair_cap, far_cap, far_base, block_len, kv_heads, n_new, levels = cfg
    n_group = n_dev // FIND_STEP
    group_blocks = per_dev // n_group
    perm = permutation(block_len * kv_heads, lambda r: lax.rem(r, block_len) * kv_heads + r // block_len)

    def group_copies(group):
        rows = pl.ds(group * group_blocks, group_blocks)
        return [pltpu.make_async_copy(src.at[rows], raw.at[i, rows], in_sem.at[i, group])
                for i, src in enumerate((k_pool, v_pool))]

    new_in = [pltpu.make_async_copy(src, new_buf.at[i], new_sem.at[i]) for i, src in enumerate((k_new, v_new))]
    pool_out = [pltpu.make_async_copy(raw.at[i], dst, pool_sem.at[i]) for i, dst in enumerate((k_out, v_out))]
    for group in range(n_group):
        for copy in group_copies(group):
            copy.start()
    for copy in new_in:
        copy.start()
    n_cols = n_dev // PLANES
    n_pref, n_entry = table_in.shape[0], table.shape[1]
    n_req = n_entry // n_pref
    by_row[...] = table_in[...].T
    for r in range(n_req):
        table[:, r * n_pref:(r + 1) * n_pref] = by_row[pl.ds(r, n_dev, stride=n_req), :]
    me = lax.axis_index('pool')
    half, in_half = me // n_half, lax.rem(me, n_half)
    partner = (1 - half) * n_half + in_half
    plane, col = me // n_cols, lax.rem(me, n_cols)
    tri = flag(iota((per_dev, per_dev), 0) < iota((per_dev, per_dev), 1)).astype(BF16)
    rowsum = lambda x: jnp.sum(x, axis=1, keepdims=True)

    def hot_entries(dest):
        row = table[pl.ds(dest, 1), :]
        owner = row // per_dev
        return (flag(iota((n_dev, n_entry), 0) == owner).astype(BF16),
                flag(iota((per_dev, n_entry), 0) == row - owner * per_dev).astype(BF16))

    def find(dest, popular):
        by_owner, by_block = hot_entries(dest)
        hits = lax.dot_general(by_owner, by_block, (((1,), (1,)), ((), ())), preferred_element_type=F32)
        want = flag(hits > 0)
        want_s[dest] = want
        return popular + want

    def find_and_turn(group, popular):
        for copy in group_copies(group):
            copy.wait()
        for i in range(FIND_STEP):
            popular = find(group * FIND_STEP + i, popular)
            for j in range(group_blocks // FIND_STEP):
                block = group * group_blocks + i * (group_blocks // FIND_STEP) + j
                turned = dot_nn(perm, jnp.concatenate([raw[0, block], raw[1, block]], axis=1)).astype(BF16)
                head_major[block, 0:128, :] = turned[:, 0:128]
                head_major[block, 128:256, :] = turned[:, 128:256]
        return popular
    popular = lax.fori_loop(0, n_group, find_and_turn, jnp.zeros((n_dev, per_dev), F32))
    for copy in pool_out:
        copy.start()

    def search(_, bounds):
        low, high = bounds
        mid = (low + high) // 2
        fits = jnp.sum(flag(popular >= mid.astype(F32))) <= HOT_CAP
        return jnp.where(fits, low, mid + 1), jnp.where(fits, mid, high)
    steps = n_dev.bit_length()
    threshold, _ = lax.fori_loop(0, steps, search, (jnp.int32(2), jnp.int32(n_dev + 1)))
    hot = flag(popular >= threshold.astype(F32))
    hot_rank = dot_nn(hot, tri)
    hot = hot * flag(hot_rank < 2 * HOT_PART)
    hot_half = jnp.floor(hot_rank * 0.5)
    hot_part = hot_rank - 2 * hot_half
    hot_of = [hot * flag(hot_part == p) for p in range(2)]
    for p in range(2):
        hot_s[p] = hot_of[p]
    hot_s[2] = hot_half

    def rank_rest(dest, carry):
        union, pair_max, far_max = carry
        want = want_s[dest]
        rest = want * (1 - hot)
        key_s[dest] = jnp.where(rest > 0, dot_nn(rest, tri), -1.0)
        num = rowsum(rest)
        count_s[dest] = jnp.broadcast_to(num, (n_dev, 128))
        held = []
        for p in range(2):
            per_owner = rowsum(want * hot_of[p])
            held.append(sum(per_owner[q * n_cols:(q + 1) * n_cols] for q in range(PLANES)))
        across = jnp.where(dest < n_half, num[n_half:], num[:n_half])
        far = across + jnp.concatenate(held, axis=0)
        return jnp.maximum(union, rest), jnp.maximum(pair_max, num), jnp.maximum(far_max, far)

    def rank_half(first, maxima):
        zero = jnp.zeros((n_dev, per_dev), F32)

        def several(step, carry):
            for i in range(FIND_STEP):
                carry = rank_rest(first + step * FIND_STEP + i, carry)
            return carry
        return lax.fori_loop(0, n_half // FIND_STEP, several, (zero,) + maxima)
    union0, pair_max, far_max = rank_half(0, (jnp.zeros((n_dev, 1), F32), jnp.zeros((n_half, 1), F32)))
    union1, pair_max, far_max = rank_half(n_half, (pair_max, far_max))
    for h, union in enumerate((union0, union1)):
        union_s[h] = jnp.where(union > 0, dot_nn(union, tri), -1.0)
    union_max = jnp.maximum(jnp.max(rowsum(union0)[n_half:]), jnp.max(rowsum(union1)[:n_half]))
    pair_max, far_max = jnp.max(pair_max), jnp.max(far_max)
    level = jnp.int32(0)
    for near_send, n_cross, far_send in levels:
        over = (pair_max > near_send) | (union_max > n_cross) | (far_max > far_send)
        level = level + over.astype(jnp.int32)
    out[LEVEL_ROW:LEVEL_ROW + 1, :] = jnp.full((1, per_dev), level, jnp.int32)

    def compact(keys, values, size):
        places = iota((size, per_dev), 0).astype(F32)
        hits = jnp.concatenate([flag(key == places).astype(BF16) for key in keys], axis=1)
        values = jnp.broadcast_to(jnp.concatenate(values, axis=1), (8, per_dev * len(keys))).astype(BF16)
        ids = lax.dot_general(values, hits, (((1,), (1,)), ((), ())), preferred_element_type=F32)
        return ids[0:1]

    def put(row, ids, num):
        out[row:row + 1, 0:ids.shape[1]] = ids.astype(jnp.int32)
        if ids.shape[1] < per_dev:
            out[row:row + 1, COUNT_LANE:] = jnp.broadcast_to(num, (1, per_dev - COUNT_LANE)).astype(jnp.int32)

    ids = iota((1, per_dev), 1).astype(F32)
    dests = [half * n_half + d for d in range(n_half)]
    stack = lambda ref, at: jnp.concatenate([ref[d, pl.ds(at, 1), :] for d in dests], axis=0)
    near_keys = stack(key_s, me)
    relay_keys = [stack(key_s, partner)]
    relay_num = [rowsum(flag(relay_keys[0] >= 0))]
    mine = lax.rem(plane, 2)
    for q in range(PLANES):
        here = stack(want_s, q * n_cols + col) * hot_s[mine, pl.ds(q * n_cols + col, 1), :]
        before = sum(relay_num)
        relay_keys.append(jnp.where(here > 0, dot_nn(here, tri) + before, -1.0))
        relay_num.append(rowsum(here))
    relay_at = [union_s[half, pl.ds(partner, 1), :]]
    for q in range(PLANES):
        relay_at.append(q * HOT_PART + hot_s[2, pl.ds(q * n_cols + col, 1), :])
    cross_key = union_s[1 - half, pl.ds(me, 1), :]
    hot_keys = [jnp.where(hot_s[p, pl.ds(me, 1), :] > 0, hot_s[2, pl.ds(me, 1), :], -1.0) for p in range(2)]
    near_num = rowsum(flag(near_keys >= 0))
    for d in range(n_half):
        put(NEAR_ROW + d, compact([near_keys[d:d + 1]], [ids], LIST_LANES), near_num[d:d + 1])
        listed = compact([keys[d:d + 1] for keys in relay_keys], relay_at, LIST_LANES)
        from_partner = flag(iota((1, LIST_LANES), 1).astype(F32) < relay_num[0][d:d + 1])
        put(RELAY_ROW + d, listed + HOT_IN * from_partner, sum(relay_num)[d:d + 1])
    put(CROSS_ROW, compact([cross_key], [ids], per_dev), None)
    for p in range(2):
        put(HOT_ROW + p, compact([hot_keys[p]], [ids], LIST_LANES), rowsum(flag(hot_keys[p] >= 0)))
    cross_num = rowsum(flag(cross_key >= 0)).astype(jnp.int32)
    out[LEVEL_ROW:LEVEL_ROW + 1, COUNT_LANE:] = jnp.broadcast_to(cross_num, (1, per_dev - COUNT_LANE))

    owner = iota((n_dev, 1), 0)
    group = lax.rem(owner, n_half).astype(F32)
    is_near = owner // n_half == half
    rest_at = jnp.where(is_near, group * pair_cap, far_base + group * far_cap) + key_s[me]
    num = count_s[me, :, 0:1]
    across = jnp.where(half == 0, num[n_half:], num[:n_half])
    place = rest_at
    for p in range(2):
        here = want_s[me] * hot_of[p]
        per_owner = rowsum(here)
        parts = [per_owner[q * n_cols:(q + 1) * n_cols] for q in range(PLANES)]
        holder = p * n_cols + iota((n_cols, 1), 0)
        start = far_base + holder.astype(F32) * far_cap + across[p * n_cols:(p + 1) * n_cols]
        starts = [start]
        for part in parts[:-1]:
            starts.append(starts[-1] + part)
        place = jnp.where(here > 0, jnp.concatenate(starts, axis=0) + dot_nn(here, tri), place)
    place = jnp.maximum(place, 0.0)
    high = jnp.floor(place * (1.0 / 256))
    by_owner, by_block = hot_entries(me)
    picked = dot_nn(high, by_block) * 256 + dot_nn(place - high * 256, by_block)
    pos = jnp.sum(picked * by_owner.astype(F32), axis=0, keepdims=True).astype(jnp.int32)
    for i in range(n_entry // per_dev):
        out[POS_ROW + i:POS_ROW + i + 1, :] = pos[:, i * per_dev:(i + 1) * per_dev]

    to_scalar = pltpu.make_async_copy(out, plan, plan_sem)
    to_scalar.start()
    to_scalar.wait()

    def start_list(row, count, dest, base):
        def body(k, carry):
            pltpu.make_async_copy(head_major.at[plan[row, k]], dest.at[base + k], out_sem).start()
            return carry
        lax.fori_loop(0, count, body, 0)

    total = plan[LEVEL_ROW, COUNT_LANE]
    start_list(CROSS_ROW, total, x_cross, 0)
    for q in range(2):
        count = plan[HOT_ROW + q, COUNT_LANE]
        start_list(HOT_ROW + q, count, x_hot, q * HOT_PART)
        total = total + count
    for q in range(n_half):
        count = plan[NEAR_ROW + q, COUNT_LANE]
        start_list(NEAR_ROW + q, count, x_near, q * pair_cap)
        total = total + count

    for copy in pool_out + new_in:
        copy.wait()

    def new_copies(i):
        return [pltpu.make_async_copy(new_buf.at[which, i], dst.at[targets[i % targets.shape[0], i // targets.shape[0]]], new_sem.at[which])
                for which, dst in enumerate((k_out, v_out))]

    for i in range(n_new):
        for copy in new_copies(i):
            copy.start()

    def drain(k, carry):
        pltpu.make_async_copy(head_major.at[0], x_near.at[0], out_sem).wait()
        return carry
    lax.fori_loop(0, total, drain, 0)
    for i in range(n_new):
        for copy in new_copies(i):
            copy.wait()


def pack_relay_kernel(cfg, plan, arrived, x_out, stage, in_sem, out_sem):
    n_half, far_cap, n_arrived = cfg

    whole = pltpu.make_async_copy(arrived, stage, in_sem)
    whole.start()
    whole.wait()
    total = 0
    for q in range(n_half):
        def store(k, carry, q=q):
            pltpu.make_async_copy(stage.at[plan[RELAY_ROW + q, k]], x_out.at[q * far_cap + k], out_sem).start()
            return carry
        num = plan[RELAY_ROW + q, COUNT_LANE]
        lax.fori_loop(0, num, store, 0)
        total = total + num

    def drain(k, carry):
        pltpu.make_async_copy(stage.at[0], x_out.at[0], out_sem).wait()
        return carry
    lax.fori_loop(0, total, drain, 0)


def xor_bits(index, bits):
    out = index
    bit = 1
    while bit <= bits:
        if bits & bit:
            out = out + bit - 2 * bit * lax.rem(index // bit, 2)
        bit *= 2
    return out


def exchange_kernel(cfg, *refs):
    n_half, slot_cap, pair_send, n_cross, base = cfg
    first = n_cross > 0
    if first:
        x_pair, x_cross, x_hot, recv, arrived, own, send_sem, recv_sem, own_sem = refs
    else:
        x_pair, _, recv, own, send_sem, recv_sem, own_sem = refs
    me = lax.axis_index('pool')
    in_half = lax.rem(me, n_half)
    half = me // n_half
    n_cols = 2 * n_half // PLANES
    plane, col = me // n_cols, lax.rem(me, n_cols)
    own_group = recv.at[pl.ds(base + in_half * slot_cap, pair_send)]
    sends = []
    for j in ORDER:
        sends.append((half * n_half + xor_bits(in_half, j),
                      x_pair.at[pl.ds(xor_bits(in_half, j) * slot_cap, pair_send)], own_group))
    own_copies = [(x_pair.at[pl.ds(in_half * slot_cap, pair_send)], own.at[pl.ds(0, pair_send)], own_group)]
    if first:
        hot_here = arrived.at[pl.ds(plane * HOT_PART, HOT_PART)]
        hot_for = lambda p: x_hot.at[pl.ds(lax.rem(p, 2) * HOT_PART, HOT_PART)]
        sends.append(((1 - half) * n_half + in_half, x_cross.at[pl.ds(0, n_cross)],
                      arrived.at[pl.ds(HOT_IN, n_cross)]))
        for j in range(1, PLANES):
            to = xor_bits(plane, j)
            sends.append((to * n_cols + col, hot_for(to), hot_here))
        own_copies.append((hot_for(plane), own.at[pl.ds(pair_send, HOT_PART)], hot_here))

    barrier = pltpu.get_barrier_semaphore()
    for peer, _, _ in sends:
        pl.semaphore_signal(barrier, inc=1, device_id=(peer,), device_id_type=MESH)
    own_in = [pltpu.make_async_copy(src, mid, own_sem.at[0, i]) for i, (src, mid, _) in enumerate(own_copies)]
    for copy in own_in:
        copy.start()
    pl.semaphore_wait(barrier, len(sends))
    copies = []
    for i, (peer, src, dst) in enumerate(sends):
        copies.append(pltpu.make_async_remote_copy(
            src_ref=src, dst_ref=dst, send_sem=send_sem.at[i], recv_sem=recv_sem.at[i],
            device_id=(peer,), device_id_type=MESH))
        copies[-1].start()
    for copy in own_in:
        copy.wait()
    own_out = [pltpu.make_async_copy(mid, dst, own_sem.at[1, i]) for i, (_, mid, dst) in enumerate(own_copies)]
    for copy in own_out:
        copy.start()
    for copy in own_out + copies:
        copy.wait()


def attend_kernel(cfg, plan, q_ref, kn_ref, vn_ref, recv, out_ref,
                  kv, q_heads, heads_out, new_heads_kv, s_pref, s_self, p_pref, p_self, sem):
    n_pref, block_len, kv_heads, groups, chunk_len, head_dim, n_req, per_dev = cfg
    req = pl.program_id(0)
    slot = lax.rem(req, 2)
    exp_scale = float(head_dim ** -0.5 * 1.4426950408889634)
    per_row = per_dev // n_pref

    def fetch(which, into, first, num):
        row, lane = POS_ROW + which // per_row, lax.rem(which, per_row) * n_pref
        for k in range(num):
            pltpu.make_async_copy(recv.at[plan[row, lane + first + k]], kv.at[into, first + k], sem.at[into]).start()

    @pl.when(req == 0)
    def _():
        fetch(0, 0, 0, n_pref)

    def whole_request(at):
        return pltpu.make_async_copy(recv.at[pl.ds(0, n_pref)], kv.at[at], sem.at[at])

    whole_request(slot).wait()
    aligned = lambda i, n: pl.multiple_of(i * n, n)

    rows = chunk_len * groups
    token = lax.broadcasted_iota(jnp.int32, (rows, chunk_len), 0) // groups
    causal = lax.broadcasted_iota(jnp.int32, (rows, chunk_len), 1) <= token
    n_keys = n_pref * block_len
    nt = (((1,), (1,)), ((), ()))
    span = 256 // kv_heads
    span_tok = span // groups
    to_heads = permutation(256, lambda r: lax.rem(r // groups, span_tok) * (kv_heads * groups)
                           + r // span * groups + lax.rem(r, groups))
    to_tokens = permutation(256, lambda r: lax.rem(r // groups, kv_heads) * span
                            + r // (kv_heads * groups) * groups + lax.rem(r, groups))
    new_heads = permutation(256, lambda r: lax.rem(r, chunk_len) * kv_heads + r // chunk_len)
    for g in range(rows // span):
        part = jnp.dot(to_heads, q_ref[0, g * 256:(g + 1) * 256, :], preferred_element_type=F32).astype(BF16)
        for h in range(kv_heads):
            q_heads[h, g * span:(g + 1) * span, :] = part[h * span:(h + 1) * span]
    new_kv = jnp.concatenate([kn_ref[0], vn_ref[0]], axis=1)
    new_heads_kv[...] = jnp.dot(new_heads, new_kv, preferred_element_type=F32).astype(BF16)
    def scores(h, at):
        k_h = kv[slot, :, pl.ds(aligned(h, block_len), block_len), :].reshape(n_keys, head_dim)
        k_own = new_heads_kv[pl.ds(aligned(h, chunk_len), chunk_len), 0:head_dim]
        s_pref[at] = lax.dot_general(q_heads[h], k_h, nt, preferred_element_type=F32)
        s_own = lax.dot_general(q_heads[h], k_own, nt, preferred_element_type=F32)
        s_self[at] = jnp.where(causal, s_own, -jnp.inf)

    def probabilities(h, at):
        for first in range(0, rows, PIECE):
            part = pl.ds(first, PIECE)
            far, own = s_pref[at, part], s_self[at, part]
            row_max = jnp.maximum(jnp.max(far, axis=-1, keepdims=True), jnp.max(own, axis=-1, keepdims=True))
            far = jnp.exp2((far - row_max) * exp_scale)
            own = jnp.exp2((own - row_max) * exp_scale)
            inv = 1.0 / (jnp.sum(far, axis=-1, keepdims=True) + jnp.sum(own, axis=-1, keepdims=True))
            p_pref[at, part] = (far * inv).astype(BF16)
            p_self[at, part] = (own * inv).astype(BF16)

    def values(h, at):
        v_h = kv[slot, :, pl.ds(aligned(kv_heads + h, block_len), block_len), :].reshape(n_keys, head_dim)
        v_own = new_heads_kv[pl.ds(aligned(h, chunk_len), chunk_len), head_dim:]
        acc = jnp.dot(p_pref[at], v_h, preferred_element_type=F32)
        acc = acc + jnp.dot(p_self[at], v_own, preferred_element_type=F32)
        heads_out[h] = acc.astype(BF16)

    n_part = n_pref // kv_heads
    after = jnp.minimum(req + 1, n_req - 1)

    fetch(after, 1 - slot, 0, n_part)
    scores(0, 0)
    fetch(after, 1 - slot, n_part, n_part)
    scores(1, 1)
    probabilities(0, 0)

    def steady(pair, carry):
        for at in range(2):
            h = 2 * pair + at
            fetch(after, 1 - slot, h * n_part, n_part)
            scores(h, at)
            probabilities(h - 1, 1 - at)
            values(h - 2, at)
        return carry
    lax.fori_loop(1, kv_heads // 2, steady, 0)
    probabilities(kv_heads - 1, 1)
    values(kv_heads - 2, 0)
    values(kv_heads - 1, 1)
    for g in range(rows // span):
        part = heads_out[:, g * span:(g + 1) * span, :].reshape(256, head_dim)
        out_ref[0, g * 256:(g + 1) * 256, :] = jnp.dot(to_tokens, part, preferred_element_type=F32).astype(BF16)

    @pl.when(req == n_req - 1)
    def _():
        whole_request(1 - slot).wait()


def solution(mesh):
    n_dev = mesh.shape['pool']

    def local_step(queries, k_new, v_new, k_pool, v_pool, block_table, write_ids):
        req_count, chunk_len, q_heads, head_dim = queries.shape
        kv_heads = k_new.shape[2]
        groups = q_heads // kv_heads
        per_dev, block_len = k_pool.shape[0], k_pool.shape[1]
        n_pref = block_table.shape[1]
        block_rows = block_len * kv_heads
        pair_cap = req_count * ROW_CAP
        n_half = n_dev // 2
        rows = chunk_len * groups
        n_cols = n_dev // PLANES
        far_cap = pair_cap + HOT_IN
        far_base = n_half * pair_cap
        n_recv = far_base + n_half * far_cap
        block_shape = (2 * block_rows, head_dim)
        shaped = lambda n: jax.ShapeDtypeStruct((n,) + block_shape, BF16)
        flat_pool = (per_dev, block_rows, head_dim)
        new_shape = (write_ids.size, block_rows, head_dim)
        k_flat, v_flat = k_pool.reshape(flat_pool), v_pool.reshape(flat_pool)
        plan, x_near, x_cross, x_hot, k_pool_out, v_pool_out = pl.pallas_call(
            functools.partial(plan_kernel, (n_dev, n_half, per_dev, pair_cap, far_cap, far_base, block_len,
                                            kv_heads, write_ids.size, LEVELS)),
            out_shape=(jax.ShapeDtypeStruct((PLAN_ROWS, per_dev), jnp.int32),
                       shaped(n_half * pair_cap), shaped(per_dev), shaped(2 * HOT_PART),
                       jax.ShapeDtypeStruct(flat_pool, BF16), jax.ShapeDtypeStruct(flat_pool, BF16)),
            in_specs=[smem_spec(), vmem_spec()] + [any_spec()] * 4, out_specs=(vmem_spec(),) + (any_spec(),) * 5,
            scratch_shapes=[
                pltpu.VMEM(block_table.shape, jnp.int32),
                pltpu.VMEM((n_dev, req_count * n_pref), jnp.int32),
                pltpu.VMEM((n_dev, n_dev, per_dev), F32),
                pltpu.VMEM((n_dev, n_dev, per_dev), F32),
                pltpu.VMEM((3, n_dev, per_dev), F32),
                pltpu.VMEM((n_dev, n_dev, 128), F32),
                pltpu.VMEM((2, n_dev, per_dev), F32),
                pltpu.VMEM((2,) + flat_pool, BF16),
                pltpu.VMEM((per_dev,) + block_shape, BF16),
                pltpu.SMEM((PLAN_ROWS, per_dev), jnp.int32),
                pltpu.VMEM((2,) + new_shape, BF16),
                pltpu.SemaphoreType.DMA((2, n_dev // FIND_STEP)),
                pltpu.SemaphoreType.DMA((2,)),
                pltpu.SemaphoreType.DMA((2,)),
                pltpu.SemaphoreType.DMA,
                pltpu.SemaphoreType.DMA,
            ],
            compiler_params=pltpu.CompilerParams(vmem_limit_bytes=56 << 20),
            name='plan',
        )(write_ids.T, block_table.T, k_flat, v_flat,
          k_new.reshape(new_shape), v_new.reshape(new_shape))

        def exchange(level, near_send, n_cross, far_send, x_near, x_cross, x_hot, plan):
            n_arrived = HOT_IN + n_cross

            def exchange_call(first, send, out_shape, n_in, alias, name):
                n_copy = n_half + PLANES
                return pl.pallas_call(
                    functools.partial(exchange_kernel, (
                        n_half, pair_cap if first else far_cap, send, n_cross if first else 0,
                        0 if first else far_base)),
                    out_shape=out_shape, in_specs=[any_spec()] * n_in,
                    out_specs=(any_spec(),) * 2 if first else any_spec(),
                    scratch_shapes=[
                        pltpu.VMEM((send + HOT_PART,) + block_shape, BF16), pltpu.SemaphoreType.DMA((n_copy,)),
                        pltpu.SemaphoreType.DMA((n_copy,)), pltpu.SemaphoreType.DMA((2, 2))],
                    input_output_aliases=alias,
                    compiler_params=pltpu.CompilerParams(
                        collective_id=2 * level + (0 if first else 1), has_side_effects=True,
                        vmem_limit_bytes=8 << 20),
                    name=name)

            recv, arrived = exchange_call(True, near_send, (shaped(n_recv), shaped(n_arrived)), 3, {},
                                          'exchange_near')(x_near, x_cross, x_hot)
            x_relay = pl.pallas_call(
                functools.partial(pack_relay_kernel, (n_half, far_cap, n_arrived)),
                out_shape=shaped(n_half * far_cap),
                in_specs=[smem_spec(), any_spec()], out_specs=any_spec(),
                scratch_shapes=[pltpu.VMEM((n_arrived,) + block_shape, BF16), pltpu.SemaphoreType.DMA,
                                pltpu.SemaphoreType.DMA],
                compiler_params=pltpu.CompilerParams(vmem_limit_bytes=24 << 20), name='pack_relay',
            )(plan, arrived)
            return exchange_call(False, far_send, shaped(n_recv), 2, {1: 0}, 'exchange_far')(x_relay, recv)

        sizes = tuple(LEVELS) + ((pair_cap, per_dev, far_cap),)
        recv = lax.switch(plan[LEVEL_ROW, 0], [functools.partial(exchange, i, *s) for i, s in enumerate(sizes)],
                          x_near, x_cross, x_hot, plan)

        cfg = (n_pref, block_len, kv_heads, groups, chunk_len, head_dim, req_count, per_dev)
        row_block = lambda *dims: pl.BlockSpec((1,) + dims, lambda r: (r,) + (0,) * len(dims))
        attn = pl.pallas_call(
            functools.partial(attend_kernel, cfg),
            out_shape=jax.ShapeDtypeStruct((req_count, chunk_len * q_heads, head_dim), BF16),
            grid=(req_count,),
            in_specs=[
                smem_spec(), row_block(chunk_len * q_heads, head_dim),
                row_block(chunk_len * kv_heads, head_dim), row_block(chunk_len * kv_heads, head_dim), any_spec(),
            ],
            out_specs=row_block(chunk_len * q_heads, head_dim),
            scratch_shapes=[
                pltpu.VMEM((2, n_pref) + block_shape, BF16),
                pltpu.VMEM((kv_heads, rows, head_dim), BF16),
                pltpu.VMEM((kv_heads, rows, head_dim), BF16),
                pltpu.VMEM((chunk_len * kv_heads, 2 * head_dim), BF16),
                pltpu.VMEM((2, rows, n_pref * block_len), F32),
                pltpu.VMEM((2, rows, chunk_len), F32),
                pltpu.VMEM((2, rows, n_pref * block_len), BF16),
                pltpu.VMEM((2, rows, chunk_len), BF16),
                pltpu.SemaphoreType.DMA((2,)),
            ],
            compiler_params=pltpu.CompilerParams(
                vmem_limit_bytes=56 << 20, dimension_semantics=('arbitrary',)),
            name='attend',
        )(plan, queries.reshape(req_count, chunk_len * q_heads, head_dim),
          k_new.reshape(req_count, chunk_len * kv_heads, head_dim),
          v_new.reshape(req_count, chunk_len * kv_heads, head_dim), recv)
        attn_out = attn.reshape(req_count, chunk_len, q_heads, head_dim)
        return attn_out, k_pool_out.reshape(k_pool.shape), v_pool_out.reshape(v_pool.shape)

    row_spec = P('pool')
    return jax.shard_map(local_step, mesh=mesh, in_specs=(row_spec, row_spec, row_spec, row_spec, row_spec, P(), row_spec), out_specs=(row_spec, row_spec, row_spec), check_vma=False)
```

```python
import functools

import jax
import jax.numpy as jnp
from jax import lax
from jax.experimental import pallas as pl
from jax.experimental.pallas import tpu as pltpu
from jax.sharding import PartitionSpec as P

F32 = jnp.float32
BF16 = jnp.bfloat16
ROW_CAP = 5
FIND_STEP = 8
PIECE = 32
HOT_CAP = 64
PLANES = 4
HOT_PART = 4
HOT_IN = PLANES * HOT_PART
NEAR_ROW, RELAY_ROW, CROSS_ROW, HOT_ROW, LEVEL_ROW, POS_ROW, PLAN_ROWS = 0, 16, 32, 33, 35, 36, 40
COUNT_LANE = 128
LIST_LANES = 64
MESH = pl.DeviceIdType.MESH
ORDER = (14, 8, 4, 6, 12, 10, 2, 15, 9, 5, 7, 13, 11, 3, 1)
LEVELS = ((8, 54, 10), (8, 56, 10), (8, 58, 10), (8, 61, 10), (8, 64, 10), (12, 80, 16))


def any_spec():
    return pl.BlockSpec(memory_space=pl.ANY)


def smem_spec():
    return pl.BlockSpec(memory_space=pltpu.SMEM)


def vmem_spec():
    return pl.BlockSpec(memory_space=pltpu.VMEM)


def dot_nn(a, b):
    return jnp.dot(a.astype(BF16), b.astype(BF16), preferred_element_type=F32)


def flag(cond):
    return jnp.where(cond, 1.0, 0.0)


def iota(shape, dim):
    return lax.broadcasted_iota(jnp.int32, shape, dim)


def permutation(n, src_of_row):
    return flag(src_of_row(iota((n, n), 0)) == iota((n, n), 1)).astype(BF16)


def plan_kernel(cfg, targets, table_in, k_pool, v_pool, k_new, v_new, out, x_near, x_cross, x_hot, k_out, v_out,
                by_row, table, want_s, key_s, hot_s, count_s, union_s, raw, head_major, plan, new_buf,
                in_sem, pool_sem, new_sem, plan_sem, out_sem):
    n_dev, n_half, per_dev, pair_cap, far_cap, far_base, block_len, kv_heads, n_new, levels = cfg
    n_group = n_dev // FIND_STEP
    group_blocks = per_dev // n_group
    perm = permutation(block_len * kv_heads, lambda r: lax.rem(r, block_len) * kv_heads + r // block_len)

    def group_copies(group):
        rows = pl.ds(group * group_blocks, group_blocks)
        return [pltpu.make_async_copy(src.at[rows], raw.at[i, rows], in_sem.at[i, group])
                for i, src in enumerate((k_pool, v_pool))]

    new_in = [pltpu.make_async_copy(src, new_buf.at[i], new_sem.at[i]) for i, src in enumerate((k_new, v_new))]
    pool_out = [pltpu.make_async_copy(raw.at[i], dst, pool_sem.at[i]) for i, dst in enumerate((k_out, v_out))]
    for group in range(n_group):
        for copy in group_copies(group):
            copy.start()
    for copy in new_in:
        copy.start()
    n_cols = n_dev // PLANES
    n_pref, n_entry = table_in.shape[0], table.shape[1]
    n_req = n_entry // n_pref
    by_row[...] = table_in[...].T
    for r in range(n_req):
        table[:, r * n_pref:(r + 1) * n_pref] = by_row[pl.ds(r, n_dev, stride=n_req), :]
    me = lax.axis_index('pool')
    half, in_half = me // n_half, lax.rem(me, n_half)
    partner = (1 - half) * n_half + in_half
    plane, col = me // n_cols, lax.rem(me, n_cols)
    tri = flag(iota((per_dev, per_dev), 0) < iota((per_dev, per_dev), 1)).astype(BF16)
    rowsum = lambda x: jnp.sum(x, axis=1, keepdims=True)

    def hot_entries(dest):
        row = table[pl.ds(dest, 1), :]
        owner = row // per_dev
        return (flag(iota((n_dev, n_entry), 0) == owner).astype(BF16),
                flag(iota((per_dev, n_entry), 0) == row - owner * per_dev).astype(BF16))

    def find(dest, popular):
        by_owner, by_block = hot_entries(dest)
        hits = lax.dot_general(by_owner, by_block, (((1,), (1,)), ((), ())), preferred_element_type=F32)
        want = flag(hits > 0)
        want_s[dest] = want
        return popular + want

    def find_and_turn(group, popular):
        for copy in group_copies(group):
            copy.wait()
        for i in range(FIND_STEP):
            popular = find(group * FIND_STEP + i, popular)
            for j in range(group_blocks // FIND_STEP):
                block = group * group_blocks + i * (group_blocks // FIND_STEP) + j
                turned = dot_nn(perm, jnp.concatenate([raw[0, block], raw[1, block]], axis=1)).astype(BF16)
                head_major[block, 0:128, :] = turned[:, 0:128]
                head_major[block, 128:256, :] = turned[:, 128:256]
        return popular
    popular = lax.fori_loop(0, n_group, find_and_turn, jnp.zeros((n_dev, per_dev), F32))
    for copy in pool_out:
        copy.start()

    def search(_, bounds):
        low, high = bounds
        mid = (low + high) // 2
        fits = jnp.sum(flag(popular >= mid.astype(F32))) <= HOT_CAP
        return jnp.where(fits, low, mid + 1), jnp.where(fits, mid, high)
    steps = n_dev.bit_length()
    threshold, _ = lax.fori_loop(0, steps, search, (jnp.int32(2), jnp.int32(n_dev + 1)))
    hot = flag(popular >= threshold.astype(F32))
    hot_rank = dot_nn(hot, tri)
    hot = hot * flag(hot_rank < 2 * HOT_PART)
    hot_half = jnp.floor(hot_rank * 0.5)
    hot_part = hot_rank - 2 * hot_half
    hot_of = [hot * flag(hot_part == p) for p in range(2)]
    for p in range(2):
        hot_s[p] = hot_of[p]
    hot_s[2] = hot_half

    def rank_rest(dest, carry):
        union, pair_max, far_max = carry
        want = want_s[dest]
        rest = want * (1 - hot)
        key_s[dest] = jnp.where(rest > 0, dot_nn(rest, tri), -1.0)
        num = rowsum(rest)
        count_s[dest] = jnp.broadcast_to(num, (n_dev, 128))
        held = []
        for p in range(2):
            per_owner = rowsum(want * hot_of[p])
            held.append(sum(per_owner[q * n_cols:(q + 1) * n_cols] for q in range(PLANES)))
        across = jnp.where(dest < n_half, num[n_half:], num[:n_half])
        far = across + jnp.concatenate(held, axis=0)
        return jnp.maximum(union, rest), jnp.maximum(pair_max, num), jnp.maximum(far_max, far)

    def rank_half(first, maxima):
        zero = jnp.zeros((n_dev, per_dev), F32)

        def several(step, carry):
            for i in range(FIND_STEP):
                carry = rank_rest(first + step * FIND_STEP + i, carry)
            return carry
        return lax.fori_loop(0, n_half // FIND_STEP, several, (zero,) + maxima)
    union0, pair_max, far_max = rank_half(0, (jnp.zeros((n_dev, 1), F32), jnp.zeros((n_half, 1), F32)))
    union1, pair_max, far_max = rank_half(n_half, (pair_max, far_max))
    for h, union in enumerate((union0, union1)):
        union_s[h] = jnp.where(union > 0, dot_nn(union, tri), -1.0)
    union_max = jnp.maximum(jnp.max(rowsum(union0)[n_half:]), jnp.max(rowsum(union1)[:n_half]))
    pair_max, far_max = jnp.max(pair_max), jnp.max(far_max)
    level = jnp.int32(0)
    for near_send, n_cross, far_send in levels:
        over = (pair_max > near_send) | (union_max > n_cross) | (far_max > far_send)
        level = level + over.astype(jnp.int32)
    out[LEVEL_ROW:LEVEL_ROW + 1, :] = jnp.full((1, per_dev), level, jnp.int32)

    def compact(keys, values, size):
        places = iota((size, per_dev), 0).astype(F32)
        hits = jnp.concatenate([flag(key == places).astype(BF16) for key in keys], axis=1)
        values = jnp.broadcast_to(jnp.concatenate(values, axis=1), (8, per_dev * len(keys))).astype(BF16)
        ids = lax.dot_general(values, hits, (((1,), (1,)), ((), ())), preferred_element_type=F32)
        return ids[0:1]

    def put(row, ids, num):
        out[row:row + 1, 0:ids.shape[1]] = ids.astype(jnp.int32)
        if ids.shape[1] < per_dev:
            out[row:row + 1, COUNT_LANE:] = jnp.broadcast_to(num, (1, per_dev - COUNT_LANE)).astype(jnp.int32)

    ids = iota((1, per_dev), 1).astype(F32)
    dests = [half * n_half + d for d in range(n_half)]
    stack = lambda ref, at: jnp.concatenate([ref[d, pl.ds(at, 1), :] for d in dests], axis=0)
    near_keys = stack(key_s, me)
    relay_keys = [stack(key_s, partner)]
    relay_num = [rowsum(flag(relay_keys[0] >= 0))]
    mine = lax.rem(plane, 2)
    for q in range(PLANES):
        here = stack(want_s, q * n_cols + col) * hot_s[mine, pl.ds(q * n_cols + col, 1), :]
        before = sum(relay_num)
        relay_keys.append(jnp.where(here > 0, dot_nn(here, tri) + before, -1.0))
        relay_num.append(rowsum(here))
    relay_at = [union_s[half, pl.ds(partner, 1), :]]
    for q in range(PLANES):
        relay_at.append(q * HOT_PART + hot_s[2, pl.ds(q * n_cols + col, 1), :])
    cross_key = union_s[1 - half, pl.ds(me, 1), :]
    hot_keys = [jnp.where(hot_s[p, pl.ds(me, 1), :] > 0, hot_s[2, pl.ds(me, 1), :], -1.0) for p in range(2)]
    near_num = rowsum(flag(near_keys >= 0))
    for d in range(n_half):
        put(NEAR_ROW + d, compact([near_keys[d:d + 1]], [ids], LIST_LANES), near_num[d:d + 1])
        listed = compact([keys[d:d + 1] for keys in relay_keys], relay_at, LIST_LANES)
        from_partner = flag(iota((1, LIST_LANES), 1).astype(F32) < relay_num[0][d:d + 1])
        put(RELAY_ROW + d, listed + HOT_IN * from_partner, sum(relay_num)[d:d + 1])
    put(CROSS_ROW, compact([cross_key], [ids], per_dev), None)
    for p in range(2):
        put(HOT_ROW + p, compact([hot_keys[p]], [ids], LIST_LANES), rowsum(flag(hot_keys[p] >= 0)))
    cross_num = rowsum(flag(cross_key >= 0)).astype(jnp.int32)
    out[LEVEL_ROW:LEVEL_ROW + 1, COUNT_LANE:] = jnp.broadcast_to(cross_num, (1, per_dev - COUNT_LANE))

    owner = iota((n_dev, 1), 0)
    group = lax.rem(owner, n_half).astype(F32)
    is_near = owner // n_half == half
    rest_at = jnp.where(is_near, group * pair_cap, far_base + group * far_cap) + key_s[me]
    num = count_s[me, :, 0:1]
    across = jnp.where(half == 0, num[n_half:], num[:n_half])
    place = rest_at
    for p in range(2):
        here = want_s[me] * hot_of[p]
        per_owner = rowsum(here)
        parts = [per_owner[q * n_cols:(q + 1) * n_cols] for q in range(PLANES)]
        holder = p * n_cols + iota((n_cols, 1), 0)
        start = far_base + holder.astype(F32) * far_cap + across[p * n_cols:(p + 1) * n_cols]
        starts = [start]
        for part in parts[:-1]:
            starts.append(starts[-1] + part)
        place = jnp.where(here > 0, jnp.concatenate(starts, axis=0) + dot_nn(here, tri), place)
    place = jnp.maximum(place, 0.0)
    high = jnp.floor(place * (1.0 / 256))
    by_owner, by_block = hot_entries(me)
    picked = dot_nn(high, by_block) * 256 + dot_nn(place - high * 256, by_block)
    pos = jnp.sum(picked * by_owner.astype(F32), axis=0, keepdims=True).astype(jnp.int32)
    for i in range(n_entry // per_dev):
        out[POS_ROW + i:POS_ROW + i + 1, :] = pos[:, i * per_dev:(i + 1) * per_dev]

    to_scalar = pltpu.make_async_copy(out, plan, plan_sem)
    to_scalar.start()
    to_scalar.wait()

    def start_list(row, count, dest, base):
        def body(k, carry):
            pltpu.make_async_copy(head_major.at[plan[row, k]], dest.at[base + k], out_sem).start()
            return carry
        lax.fori_loop(0, count, body, 0)

    total = plan[LEVEL_ROW, COUNT_LANE]
    start_list(CROSS_ROW, total, x_cross, 0)
    for q in range(2):
        count = plan[HOT_ROW + q, COUNT_LANE]
        start_list(HOT_ROW + q, count, x_hot, q * HOT_PART)
        total = total + count
    for q in range(n_half):
        count = plan[NEAR_ROW + q, COUNT_LANE]
        start_list(NEAR_ROW + q, count, x_near, q * pair_cap)
        total = total + count

    for copy in pool_out + new_in:
        copy.wait()

    def new_copies(i):
        return [pltpu.make_async_copy(new_buf.at[which, i], dst.at[targets[i % targets.shape[0], i // targets.shape[0]]], new_sem.at[which])
                for which, dst in enumerate((k_out, v_out))]

    for i in range(n_new):
        for copy in new_copies(i):
            copy.start()

    def drain(k, carry):
        pltpu.make_async_copy(head_major.at[0], x_near.at[0], out_sem).wait()
        return carry
    lax.fori_loop(0, total, drain, 0)
    for i in range(n_new):
        for copy in new_copies(i):
            copy.wait()


def pack_relay_kernel(cfg, plan, arrived, x_out, stage, in_sem, out_sem):
    n_half, far_cap, n_arrived = cfg

    whole = pltpu.make_async_copy(arrived, stage, in_sem)
    whole.start()
    whole.wait()
    total = 0
    for q in range(n_half):
        def store(k, carry, q=q):
            pltpu.make_async_copy(stage.at[plan[RELAY_ROW + q, k]], x_out.at[q * far_cap + k], out_sem).start()
            return carry
        num = plan[RELAY_ROW + q, COUNT_LANE]
        lax.fori_loop(0, num, store, 0)
        total = total + num

    def drain(k, carry):
        pltpu.make_async_copy(stage.at[0], x_out.at[0], out_sem).wait()
        return carry
    lax.fori_loop(0, total, drain, 0)


def xor_bits(index, bits):
    out = index
    bit = 1
    while bit <= bits:
        if bits & bit:
            out = out + bit - 2 * bit * lax.rem(index // bit, 2)
        bit *= 2
    return out


def exchange_kernel(cfg, *refs):
    n_half, slot_cap, pair_send, n_cross, base = cfg
    first = n_cross > 0
    if first:
        x_pair, x_cross, x_hot, recv, arrived, own, send_sem, recv_sem, own_sem = refs
    else:
        x_pair, _, recv, own, send_sem, recv_sem, own_sem = refs
    me = lax.axis_index('pool')
    in_half = lax.rem(me, n_half)
    half = me // n_half
    n_cols = 2 * n_half // PLANES
    plane, col = me // n_cols, lax.rem(me, n_cols)
    own_group = recv.at[pl.ds(base + in_half * slot_cap, pair_send)]
    sends = []
    for j in ORDER:
        sends.append((half * n_half + xor_bits(in_half, j),
                      x_pair.at[pl.ds(xor_bits(in_half, j) * slot_cap, pair_send)], own_group))
    own_copies = [(x_pair.at[pl.ds(in_half * slot_cap, pair_send)], own.at[pl.ds(0, pair_send)], own_group)]
    if first:
        hot_here = arrived.at[pl.ds(plane * HOT_PART, HOT_PART)]
        hot_for = lambda p: x_hot.at[pl.ds(lax.rem(p, 2) * HOT_PART, HOT_PART)]
        sends.append(((1 - half) * n_half + in_half, x_cross.at[pl.ds(0, n_cross)],
                      arrived.at[pl.ds(HOT_IN, n_cross)]))
        for j in range(1, PLANES):
            to = xor_bits(plane, j)
            sends.append((to * n_cols + col, hot_for(to), hot_here))
        own_copies.append((hot_for(plane), own.at[pl.ds(pair_send, HOT_PART)], hot_here))

    if first:
        near, cross, hots = sends[:n_half - 1], sends[n_half - 1:n_half], sends[n_half:]
        sends = near[:8] + cross + hots + near[8:]
    barrier = pltpu.get_barrier_semaphore()
    for peer, _, _ in sends:
        pl.semaphore_signal(barrier, inc=1, device_id=(peer,), device_id_type=MESH)
    own_in = [pltpu.make_async_copy(src, mid, own_sem.at[0, i]) for i, (src, mid, _) in enumerate(own_copies)]
    for copy in own_in:
        copy.start()
    pl.semaphore_wait(barrier, len(sends))
    copies = []
    for i, (peer, src, dst) in enumerate(sends):
        copies.append(pltpu.make_async_remote_copy(
            src_ref=src, dst_ref=dst, send_sem=send_sem.at[i], recv_sem=recv_sem.at[i],
            device_id=(peer,), device_id_type=MESH))
        copies[-1].start()
    for copy in own_in:
        copy.wait()
    own_out = [pltpu.make_async_copy(mid, dst, own_sem.at[1, i]) for i, (_, mid, dst) in enumerate(own_copies)]
    for copy in own_out:
        copy.start()
    for copy in own_out + copies:
        copy.wait()


def attend_kernel(cfg, plan, q_ref, kn_ref, vn_ref, recv, out_ref,
                  kv, q_heads, heads_out, new_heads_kv, s_pref, s_self, p_pref, p_self, sem):
    n_pref, block_len, kv_heads, groups, chunk_len, head_dim, n_req, per_dev = cfg
    req = pl.program_id(0)
    slot = lax.rem(req, 2)
    exp_scale = float(head_dim ** -0.5 * 1.4426950408889634)
    per_row = per_dev // n_pref

    def fetch(which, into, first, num):
        row, lane = POS_ROW + which // per_row, lax.rem(which, per_row) * n_pref
        for k in range(num):
            pltpu.make_async_copy(recv.at[plan[row, lane + first + k]], kv.at[into, first + k], sem.at[into]).start()

    @pl.when(req == 0)
    def _():
        fetch(0, 0, 0, n_pref)

    def whole_request(at):
        return pltpu.make_async_copy(recv.at[pl.ds(0, n_pref)], kv.at[at], sem.at[at])

    whole_request(slot).wait()
    aligned = lambda i, n: pl.multiple_of(i * n, n)

    rows = chunk_len * groups
    token = lax.broadcasted_iota(jnp.int32, (rows, chunk_len), 0) // groups
    causal = lax.broadcasted_iota(jnp.int32, (rows, chunk_len), 1) <= token
    n_keys = n_pref * block_len
    nt = (((1,), (1,)), ((), ()))
    span = 256 // kv_heads
    span_tok = span // groups
    to_heads = permutation(256, lambda r: lax.rem(r // groups, span_tok) * (kv_heads * groups)
                           + r // span * groups + lax.rem(r, groups))
    to_tokens = permutation(256, lambda r: lax.rem(r // groups, kv_heads) * span
                            + r // (kv_heads * groups) * groups + lax.rem(r, groups))
    new_heads = permutation(256, lambda r: lax.rem(r, chunk_len) * kv_heads + r // chunk_len)
    for g in range(rows // span):
        part = jnp.dot(to_heads, q_ref[0, g * 256:(g + 1) * 256, :], preferred_element_type=F32).astype(BF16)
        for h in range(kv_heads):
            q_heads[h, g * span:(g + 1) * span, :] = part[h * span:(h + 1) * span]
    new_kv = jnp.concatenate([kn_ref[0], vn_ref[0]], axis=1)
    new_heads_kv[...] = jnp.dot(new_heads, new_kv, preferred_element_type=F32).astype(BF16)
    def scores(h, at):
        k_h = kv[slot, :, pl.ds(aligned(h, block_len), block_len), :].reshape(n_keys, head_dim)
        k_own = new_heads_kv[pl.ds(aligned(h, chunk_len), chunk_len), 0:head_dim]
        s_pref[at] = lax.dot_general(q_heads[h], k_h, nt, preferred_element_type=F32)
        s_own = lax.dot_general(q_heads[h], k_own, nt, preferred_element_type=F32)
        s_self[at] = jnp.where(causal, s_own, -jnp.inf)

    def probabilities(h, at):
        for first in range(0, rows, PIECE):
            part = pl.ds(first, PIECE)
            far, own = s_pref[at, part], s_self[at, part]
            row_max = jnp.maximum(jnp.max(far, axis=-1, keepdims=True), jnp.max(own, axis=-1, keepdims=True))
            far = jnp.exp2((far - row_max) * exp_scale)
            own = jnp.exp2((own - row_max) * exp_scale)
            inv = 1.0 / (jnp.sum(far, axis=-1, keepdims=True) + jnp.sum(own, axis=-1, keepdims=True))
            p_pref[at, part] = (far * inv).astype(BF16)
            p_self[at, part] = (own * inv).astype(BF16)

    def values(h, at):
        v_h = kv[slot, :, pl.ds(aligned(kv_heads + h, block_len), block_len), :].reshape(n_keys, head_dim)
        v_own = new_heads_kv[pl.ds(aligned(h, chunk_len), chunk_len), head_dim:]
        acc = jnp.dot(p_pref[at], v_h, preferred_element_type=F32)
        acc = acc + jnp.dot(p_self[at], v_own, preferred_element_type=F32)
        heads_out[h] = acc.astype(BF16)

    n_part = n_pref // kv_heads
    after = jnp.minimum(req + 1, n_req - 1)

    fetch(after, 1 - slot, 0, n_part)
    scores(0, 0)
    fetch(after, 1 - slot, n_part, n_part)
    scores(1, 1)
    probabilities(0, 0)

    def steady(pair, carry):
        for at in range(2):
            h = 2 * pair + at
            fetch(after, 1 - slot, h * n_part, n_part)
            scores(h, at)
            probabilities(h - 1, 1 - at)
            values(h - 2, at)
        return carry
    for pair in range(1, kv_heads // 2):
        steady(pair, 0)
    probabilities(kv_heads - 1, 1)
    values(kv_heads - 2, 0)
    values(kv_heads - 1, 1)
    for g in range(rows // span):
        part = heads_out[:, g * span:(g + 1) * span, :].reshape(256, head_dim)
        out_ref[0, g * 256:(g + 1) * 256, :] = jnp.dot(to_tokens, part, preferred_element_type=F32).astype(BF16)

    @pl.when(req == n_req - 1)
    def _():
        whole_request(1 - slot).wait()


def solution(mesh):
    n_dev = mesh.shape['pool']

    def local_step(queries, k_new, v_new, k_pool, v_pool, block_table, write_ids):
        req_count, chunk_len, q_heads, head_dim = queries.shape
        kv_heads = k_new.shape[2]
        groups = q_heads // kv_heads
        per_dev, block_len = k_pool.shape[0], k_pool.shape[1]
        n_pref = block_table.shape[1]
        block_rows = block_len * kv_heads
        pair_cap = req_count * ROW_CAP
        n_half = n_dev // 2
        rows = chunk_len * groups
        n_cols = n_dev // PLANES
        far_cap = pair_cap + HOT_IN
        far_base = n_half * pair_cap
        n_recv = far_base + n_half * far_cap
        block_shape = (2 * block_rows, head_dim)
        shaped = lambda n: jax.ShapeDtypeStruct((n,) + block_shape, BF16)
        flat_pool = (per_dev, block_rows, head_dim)
        new_shape = (write_ids.size, block_rows, head_dim)
        k_flat, v_flat = k_pool.reshape(flat_pool), v_pool.reshape(flat_pool)
        plan, x_near, x_cross, x_hot, k_pool_out, v_pool_out = pl.pallas_call(
            functools.partial(plan_kernel, (n_dev, n_half, per_dev, pair_cap, far_cap, far_base, block_len,
                                            kv_heads, write_ids.size, LEVELS)),
            out_shape=(jax.ShapeDtypeStruct((PLAN_ROWS, per_dev), jnp.int32),
                       shaped(n_half * pair_cap), shaped(per_dev), shaped(2 * HOT_PART),
                       jax.ShapeDtypeStruct(flat_pool, BF16), jax.ShapeDtypeStruct(flat_pool, BF16)),
            in_specs=[smem_spec(), vmem_spec()] + [any_spec()] * 4, out_specs=(vmem_spec(),) + (any_spec(),) * 5,
            scratch_shapes=[
                pltpu.VMEM(block_table.shape, jnp.int32),
                pltpu.VMEM((n_dev, req_count * n_pref), jnp.int32),
                pltpu.VMEM((n_dev, n_dev, per_dev), F32),
                pltpu.VMEM((n_dev, n_dev, per_dev), F32),
                pltpu.VMEM((3, n_dev, per_dev), F32),
                pltpu.VMEM((n_dev, n_dev, 128), F32),
                pltpu.VMEM((2, n_dev, per_dev), F32),
                pltpu.VMEM((2,) + flat_pool, BF16),
                pltpu.VMEM((per_dev,) + block_shape, BF16),
                pltpu.SMEM((PLAN_ROWS, per_dev), jnp.int32),
                pltpu.VMEM((2,) + new_shape, BF16),
                pltpu.SemaphoreType.DMA((2, n_dev // FIND_STEP)),
                pltpu.SemaphoreType.DMA((2,)),
                pltpu.SemaphoreType.DMA((2,)),
                pltpu.SemaphoreType.DMA,
                pltpu.SemaphoreType.DMA,
            ],
            compiler_params=pltpu.CompilerParams(vmem_limit_bytes=56 << 20),
            name='plan',
        )(write_ids.T, block_table.T, k_flat, v_flat,
          k_new.reshape(new_shape), v_new.reshape(new_shape))

        def exchange(level, near_send, n_cross, far_send, x_near, x_cross, x_hot, plan):
            n_arrived = HOT_IN + n_cross

            def exchange_call(first, send, out_shape, n_in, alias, name):
                n_copy = n_half + PLANES
                return pl.pallas_call(
                    functools.partial(exchange_kernel, (
                        n_half, pair_cap if first else far_cap, send, n_cross if first else 0,
                        0 if first else far_base)),
                    out_shape=out_shape, in_specs=[any_spec()] * n_in,
                    out_specs=(any_spec(),) * 2 if first else any_spec(),
                    scratch_shapes=[
                        pltpu.VMEM((send + HOT_PART,) + block_shape, BF16), pltpu.SemaphoreType.DMA((n_copy,)),
                        pltpu.SemaphoreType.DMA((n_copy,)), pltpu.SemaphoreType.DMA((2, 2))],
                    input_output_aliases=alias,
                    compiler_params=pltpu.CompilerParams(
                        collective_id=2 * level + (0 if first else 1), has_side_effects=True,
                        vmem_limit_bytes=8 << 20),
                    name=name)

            recv, arrived = exchange_call(True, near_send, (shaped(n_recv), shaped(n_arrived)), 3, {},
                                          'exchange_near')(x_near, x_cross, x_hot)
            x_relay = pl.pallas_call(
                functools.partial(pack_relay_kernel, (n_half, far_cap, n_arrived)),
                out_shape=shaped(n_half * far_cap),
                in_specs=[smem_spec(), any_spec()], out_specs=any_spec(),
                scratch_shapes=[pltpu.VMEM((n_arrived,) + block_shape, BF16), pltpu.SemaphoreType.DMA,
                                pltpu.SemaphoreType.DMA],
                compiler_params=pltpu.CompilerParams(vmem_limit_bytes=24 << 20), name='pack_relay',
            )(plan, arrived)
            return exchange_call(False, far_send, shaped(n_recv), 2, {1: 0}, 'exchange_far')(x_relay, recv)

        sizes = tuple(LEVELS) + ((pair_cap, per_dev, far_cap),)
        recv = lax.switch(plan[LEVEL_ROW, 0], [functools.partial(exchange, i, *s) for i, s in enumerate(sizes)],
                          x_near, x_cross, x_hot, plan)

        cfg = (n_pref, block_len, kv_heads, groups, chunk_len, head_dim, req_count, per_dev)
        row_block = lambda *dims: pl.BlockSpec((1,) + dims, lambda r: (r,) + (0,) * len(dims))
        attn = pl.pallas_call(
            functools.partial(attend_kernel, cfg),
            out_shape=jax.ShapeDtypeStruct((req_count, chunk_len * q_heads, head_dim), BF16),
            grid=(req_count,),
            in_specs=[
                smem_spec(), row_block(chunk_len * q_heads, head_dim),
                row_block(chunk_len * kv_heads, head_dim), row_block(chunk_len * kv_heads, head_dim), any_spec(),
            ],
            out_specs=row_block(chunk_len * q_heads, head_dim),
            scratch_shapes=[
                pltpu.VMEM((2, n_pref) + block_shape, BF16),
                pltpu.VMEM((kv_heads, rows, head_dim), BF16),
                pltpu.VMEM((kv_heads, rows, head_dim), BF16),
                pltpu.VMEM((chunk_len * kv_heads, 2 * head_dim), BF16),
                pltpu.VMEM((2, rows, n_pref * block_len), F32),
                pltpu.VMEM((2, rows, chunk_len), F32),
                pltpu.VMEM((2, rows, n_pref * block_len), BF16),
                pltpu.VMEM((2, rows, chunk_len), BF16),
                pltpu.SemaphoreType.DMA((2,)),
            ],
            compiler_params=pltpu.CompilerParams(
                vmem_limit_bytes=56 << 20, dimension_semantics=('arbitrary',)),
            name='attend',
        )(plan, queries.reshape(req_count, chunk_len * q_heads, head_dim),
          k_new.reshape(req_count, chunk_len * kv_heads, head_dim),
          v_new.reshape(req_count, chunk_len * kv_heads, head_dim), recv)
        attn_out = attn.reshape(req_count, chunk_len, q_heads, head_dim)
        return attn_out, k_pool_out.reshape(k_pool.shape), v_pool_out.reshape(v_pool.shape)

    row_spec = P('pool')
    return jax.shard_map(local_step, mesh=mesh, in_specs=(row_spec, row_spec, row_spec, row_spec, row_spec, P(), row_spec), out_specs=(row_spec, row_spec, row_spec), check_vma=False)
```
